32 devices in a mesh: data: 1 (over z), col: 4 (over y), row: 8 (over x, core).
Axes of the slice: x: 4, y: 4, z: 1, core: 2. Of those that a mesh axis runs over, the one named last changes fastest.
The devices are a block of a 4x4x8 slice.
Arguments:
- x_seq: bfloat16 [24, 16, 5760], P(None, 'data', 'row')
- h_init: float32 [2, 16, 5760], P(None, 'data', 'row')
- wx_l1: bfloat16 [5760, 3, 5760], P('row', None, 'col')
- whru_l1: bfloat16 [5760, 2, 5760], P('row', None, 'col')
- whn_l1: bfloat16 [5760, 5760], P('row', 'col')
- bias_l1: float32 [3, 5760], P(None, 'col')
- wx_l2: bfloat16 [5760, 3, 5760], P('row', None, 'col')
- whru_l2: bfloat16 [5760, 2, 5760], P('row', None, 'col')
- whn_l2: bfloat16 [5760, 5760], P('row', 'col')
- bias_l2: float32 [3, 5760], P(None, 'col')
Outputs:
- output 1: bfloat16 [24, 16, 5760], P(None, 'data', ('col', 'row'))
- output 2: float32 [2, 16, 5760], P(None, 'data', ('col', 'row'))
All inputs are finite; a program needn't handle non-finite values.
Results may differ from the reference program's by a relative error of at most 0.00249154.
Values are sent between devices in bfloat16 or wider.
A program may use at most 768 MiB of HBM per device.

```python
import jax
import jax.numpy as jnp
from jax import lax

SEQ_LEN = 24
BATCH_GROUP = 16
HIDDEN = 5760


def setup_inputs(seed: int = 0, part: int = 0) -> dict:
    part_key = jax.random.fold_in(jax.random.key(seed), part)
    seq_key, state_key = jax.random.split(part_key, 2)
    weight_keys = jax.random.split(jax.random.key(seed + 1), 8)
    w_scale = HIDDEN ** -0.5
    gate_shift = jnp.array([0.0, 1.5, 0.0], jnp.float32)[:, None]

    def draw_weight(key, shape):
        return (w_scale * jax.random.normal(key, shape, jnp.float32)).astype(jnp.bfloat16)

    def draw_bias(key):
        return 0.5 * jax.random.normal(key, (3, HIDDEN), jnp.float32) + gate_shift

    x_seq = jax.random.normal(seq_key, (SEQ_LEN, BATCH_GROUP, HIDDEN), jnp.float32).astype(jnp.bfloat16)
    h_init = 0.8 * jnp.tanh(jax.random.normal(state_key, (2, BATCH_GROUP, HIDDEN), jnp.float32))
    return {
        "x_seq": x_seq,
        "h_init": h_init,
        "wx_l1": draw_weight(weight_keys[0], (HIDDEN, 3, HIDDEN)),
        "whru_l1": draw_weight(weight_keys[1], (HIDDEN, 2, HIDDEN)),
        "whn_l1": draw_weight(weight_keys[2], (HIDDEN, HIDDEN)),
        "bias_l1": draw_bias(weight_keys[3]),
        "wx_l2": draw_weight(weight_keys[4], (HIDDEN, 3, HIDDEN)),
        "whru_l2": draw_weight(weight_keys[5], (HIDDEN, 2, HIDDEN)),
        "whn_l2": draw_weight(weight_keys[6], (HIDDEN, HIDDEN)),
        "bias_l2": draw_bias(weight_keys[7]),
    }


def gru_layer(in_seq, w_x, w_hru, w_hn, gate_bias, h_start):
    batch_rows = in_seq.shape[1]
    wx_flat = w_x.reshape(HIDDEN, 3 * HIDDEN)
    whru_flat = w_hru.reshape(HIDDEN, 2 * HIDDEN)

    def gru_step(h_prev, step_in):
        in_proj = jnp.dot(step_in, wx_flat, preferred_element_type=jnp.float32).reshape(batch_rows, 3, HIDDEN) + gate_bias
        rec_ru = jnp.dot(h_prev.astype(jnp.bfloat16), whru_flat, preferred_element_type=jnp.float32).reshape(batch_rows, 2, HIDDEN)
        reset_gate = jax.nn.sigmoid(in_proj[:, 0] + rec_ru[:, 0])
        update_gate = jax.nn.sigmoid(in_proj[:, 1] + rec_ru[:, 1])
        gated_h = (reset_gate * h_prev).astype(jnp.bfloat16)
        candidate = jnp.tanh(in_proj[:, 2] + jnp.dot(gated_h, w_hn, preferred_element_type=jnp.float32))
        h_next = (1.0 - update_gate) * candidate + update_gate * h_prev
        return h_next, h_next.astype(jnp.bfloat16)

    return lax.scan(gru_step, h_start, in_seq)


def reference(x_seq, h_init, wx_l1, whru_l1, whn_l1, bias_l1, wx_l2, whru_l2, whn_l2, bias_l2):
    h1_last, h1_seq = gru_layer(x_seq, wx_l1, whru_l1, whn_l1, bias_l1, h_init[0])
    h2_last, h2_seq = gru_layer(h1_seq, wx_l2, whru_l2, whn_l2, bias_l2, h_init[1])
    return h2_seq, jnp.stack([h1_last, h2_last])
```

```python
import functools

import jax
import jax.numpy as jnp
from jax import lax
from jax.experimental import pallas as pl
from jax.experimental.pallas import tpu as pltpu
from jax.sharding import PartitionSpec as P

MESH = pl.DeviceIdType.MESH
F32 = jnp.float32
BF16 = jnp.bfloat16
LANES = 128

H1, RH1, H2, RH2 = range(4)
R1, N1, R2, N2 = range(4)
XR, XU, XN, PR, PU, PN, U1, U2 = range(8)
RING = 4


def cdiv(a, b):
    return -(-a // b)


def gru_kernel(dims, *refs):
    steps, batch, rows, cols, nx, ny, chunk = dims
    (x_hbm, h0, wx1, wru1u, wru1r, wn1, b1, wx2, wru2u, wru2r, wn2, b2,
     seq_out, fin_out,
     w_own, w_blk, xb, hcat, h0s, state, ag_src, ag_buf, hs, bias, bpad,
     p_u1, p_x, p_p, p_u2, s_u1, s_x, s_p, s_u2, xu_keep, pu_keep,
     blk, out_n, out_s, fin_src, fin_buf, fblk, fin_n, fin_s,
     ld_sem, wl_sem, wsend, wrecv, bs_send, bs_recv, x_sem, i_sem,
     ag_send, ag_recv, hs_send, hs_recv, rs_send, rs_recv, f_sem, o_sem) = refs
    block = 2 * rows
    device_row = lax.axis_index("row")
    y = lax.axis_index("col")
    x = device_row // 2
    core = lax.rem(device_row, 2)

    def wrap(v, n):
        return lax.rem(v + n, n)

    def remote(src, dst, ssem, rsem, tx, tc, ty):
        return pltpu.make_async_remote_copy(
            src_ref=src, dst_ref=dst, send_sem=ssem, recv_sem=rsem,
            device_id={"row": tx * 2 + tc, "col": ty}, device_id_type=MESH,
        )

    def wait_in(dst, sem):
        pltpu.make_async_copy(dst, dst, sem).wait()

    def hop(d, n):
        return min(d, n - d)

    offsets = [(dx, dy) for dx in range(nx) for dy in range(ny) if (dx, dy) != (0, 0)]
    offsets.sort(key=lambda o: hop(o[0], nx) + hop(o[1], ny))
    dists = [hop(dx, nx) + hop(dy, ny) for dx, dy in offsets]
    groups = []
    for d in sorted(set(dists)):
        first = dists.index(d)
        groups.append((first, first + dists.count(d)))
    peers = len(offsets)

    barrier = pltpu.get_barrier_semaphore()
    for d in range(1, 2 * nx * ny):
        tr = lax.rem(device_row + d % (2 * nx), 2 * nx)
        ty = lax.rem(y + d // (2 * nx), ny)
        pl.semaphore_signal(barrier, inc=1, device_id={"row": tr, "col": ty}, device_id_type=MESH)

    moved = ((wru1r, R1), (wn1, N1), (wru2r, R2), (wn2, N2))
    kept = ((wx1.at[0], XR), (wx1.at[1], XU), (wx1.at[2], XN), (wru1u, U1),
            (wx2.at[0], PR), (wx2.at[1], PU), (wx2.at[2], PN), (wru2u, U2))

    my_rows = pl.ds(pl.multiple_of(device_row * rows, 16), rows)

    def column_slice(i):
        return pl.ds(pl.multiple_of(i * chunk, LANES), chunk)

    @pl.when(core == 0)
    def _():
        loads = []
        for src, u in kept:
            loads.append(pltpu.make_async_copy(src, w_blk.at[u, pl.ds(0, rows)], ld_sem.at[u]))
        xload = pltpu.make_async_copy(x_hbm, xb.at[0], x_sem.at[0])
        xload.start()
        for c in loads:
            c.start()
        pl.semaphore_wait(barrier, 2 * nx * ny - 1)
        for src, u in moved:
            for d in range(nx):
                tx = wrap(x + d, nx)
                remote(src.at[:, column_slice(tx)], w_own.at[u, my_rows], wsend.at[u], wrecv.at[u], tx, 1, y).start()

        @pl.when(x == y)
        def _():
            remote(h0, h0s, i_sem.at[0], i_sem.at[1], x, 1, y).start()

        xload.wait()
        wait_in(xb.at[1], x_sem.at[1])
        for u in range(8):
            loads[u].wait()
            wait_in(w_blk.at[kept[u][1], pl.ds(rows, rows)], bs_recv.at[kept[u][1]])

        def row_dot(vec, u):
            return jnp.dot(vec, w_blk[u], preferred_element_type=F32)

        def spread(src, dst, kind, slot):
            for d in range(nx):
                tx = wrap(x + d, nx)
                remote(src.at[:, :, column_slice(tx)], dst.at[slot, x], rs_send.at[kind], rs_recv.at[kind, slot], tx, 1, y).start()

        def spread_wait(src, kind):
            wait_in(src, rs_send.at[kind])

        def project(t):
            def half(g):
                return (jnp.dot(xb[0, t], w_blk[g, 0:rows], preferred_element_type=F32)
                        + jnp.dot(xb[1, t], w_blk[g, rows:block], preferred_element_type=F32))
            s_x[0, :, 0:block] = half(XR)
            s_x[1, :, 0:block] = half(XN)
            spread(s_x, p_x, 1, lax.rem(t, RING))
            xu_keep[...] = half(XU)

        s_u1[...] = jnp.zeros_like(s_u1)
        s_u2[...] = jnp.zeros_like(s_u2)
        s_x[...] = jnp.zeros_like(s_x)
        s_p[...] = jnp.zeros_like(s_p)
        project(0)

        def step(i, carry):
            wait_in(hs.at[0, 0], hs_recv.at[0, lax.rem(i, 2)])
            h1v = hs[0, lax.rem(i, 2), :, 0:block]

            @pl.when(i < steps)
            def _():
                @pl.when(i > 0)
                def _():
                    spread_wait(s_u1, 0)
                s_u1[0, :, 0:block] = row_dot(h1v, U1) + xu_keep[...]
                spread(s_u1, p_u1, 0, lax.rem(i, RING))

            @pl.when(i >= 1)
            def _():
                @pl.when(i > 1)
                def _():
                    spread_wait(s_p, 2)
                s_p[0, :, 0:block] = row_dot(h1v, PR)
                s_p[1, :, 0:block] = row_dot(h1v, PN)
                spread(s_p, p_p, 2, lax.rem(i - 1, RING))
                pu_keep[...] = row_dot(h1v, PU)
                wait_in(hs.at[1, 0], hs_recv.at[1, lax.rem(i, 2)])

                @pl.when(i > 1)
                def _():
                    spread_wait(s_u2, 3)
                s_u2[0, :, 0:block] = row_dot(hs[1, lax.rem(i, 2), :, 0:block], U2) + pu_keep[...]
                spread(s_u2, p_u2, 3, lax.rem(i - 1, RING))

            @pl.when(i + 1 < steps)
            def _():
                spread_wait(s_x, 1)
                project(i + 1)
            return carry

        lax.fori_loop(0, steps + 1, step, 0)
        spread_wait(s_u1, 0)
        spread_wait(s_x, 1)
        spread_wait(s_p, 2)
        spread_wait(s_u2, 3)
        for u in range(4):
            wait_in(w_own.at[0, pl.ds(0, nx * rows)], wsend.at[u])

        @pl.when(x == y)
        def _():
            wait_in(h0, i_sem.at[0])
        wait_in(out_s, o_sem.at[1])
        wait_in(fin_s, o_sem.at[3])
        seq_out[...] = out_s[...]
        fin_out[...] = fin_s[...]

    @pl.when(core == 1)
    def _():
        own = []
        for src, u in moved:
            own.append(pltpu.make_async_copy(src.at[:, column_slice(x)], w_own.at[u, my_rows], wl_sem.at[u]))
        for c in own:
            c.start()
        pl.semaphore_wait(barrier, 2 * nx * ny - 1)
        remote(x_hbm, xb.at[1], x_sem.at[0], x_sem.at[1], x, 0, y).start()
        for src, u in kept[:4]:
            remote(src, w_blk.at[u, pl.ds(rows, rows)], bs_send.at[u], bs_recv.at[u], x, 0, y).start()
        for src, u in moved:
            for d in range(1, nx):
                tx = wrap(x + d, nx)
                remote(src.at[:, column_slice(tx)], w_own.at[u, my_rows], wsend.at[u], wrecv.at[u], tx, 1, y).start()
        for src, u in kept[4:]:
            remote(src, w_blk.at[u, pl.ds(rows, rows)], bs_send.at[u], bs_recv.at[u], x, 0, y).start()

        for u in range(4):
            w_own[u, pl.ds(nx * block, chunk * nx - block)] = jnp.zeros((chunk * nx - block, chunk), BF16)
        bpad[...] = jnp.zeros_like(bpad)
        bpad[0, 0:3, 0:block] = b1[...]
        bpad[1, 0:3, 0:block] = b2[...]
        bias[...] = bpad[:, :, column_slice(x)]
        valid = jnp.minimum(block - x * chunk, chunk)
        keep = lax.broadcasted_iota(jnp.int32, (batch, chunk), 1) < valid

        @pl.when(x == y)
        def _():
            wait_in(h0s, i_sem.at[1])
            hcat[...] = jnp.zeros_like(hcat)
            hcat[:, :, 0:rows] = h0s[...]
            hcat[:, :, rows:block] = h0[...]
            for d in range(1, nx):
                tx = wrap(x + d, nx)
                remote(hcat.at[:, :, column_slice(tx)], state, i_sem.at[2], i_sem.at[3], tx, 1, y).start()
            state[...] = hcat[:, :, column_slice(x)]
            wait_in(hcat.at[:, :, pl.ds(0, (nx - 1) * chunk)], i_sem.at[2])

        @pl.when(x != y)
        def _():
            wait_in(state, i_sem.at[3])

        def to_all(kind):
            for k in reversed(range(peers)):
                dx, dy = offsets[k]
                g = [j for j, (a, b) in enumerate(groups) if a <= k < b][0]
                remote(ag_src.at[kind], ag_buf.at[kind, k], ag_send.at[kind], ag_recv.at[kind, g],
                       wrap(x + dx, nx), 1, wrap(y + dy, ny)).start()

        def to_blocks(layer, slot):
            for d in range(ny):
                remote(ag_src.at[H1 if layer == 0 else H2], hs.at[layer, slot, :, column_slice(x)],
                       hs_send.at[layer], hs_recv.at[layer, slot], y, 0, wrap(y + d, ny)).start()

        def sent(kind):
            wait_in(ag_buf.at[kind], ag_send.at[kind])

        def sent_blocks(layer):
            wait_in(ag_buf.at[0, pl.ds(0, ny)], hs_send.at[layer])

        def weight_rows(dx, dy):
            sx, sy = wrap(x - dx, nx), wrap(y - dy, ny)
            return pl.ds(pl.multiple_of(sy * block + sx * chunk, 32), chunk)

        def gathered_dot(kind, u, acc):
            acc = acc + jnp.dot(ag_src[kind], w_own[u, weight_rows(0, 0)], preferred_element_type=F32)
            for g, (a, b) in enumerate(groups):
                wait_in(ag_buf.at[kind, pl.ds(a, b - a)], ag_recv.at[kind, g])
                for k in range(a, b):
                    acc = acc + jnp.dot(ag_buf[kind, k], w_own[u, weight_rows(*offsets[k])], preferred_element_type=F32)
            return acc

        def partial_sum(buf, slot, g):
            total = buf[slot, 0, g]
            for s in range(1, nx):
                total = total + buf[slot, s, g]
            return total

        def wait_weights(u):
            own[u].wait()
            wait_in(w_own.at[u, pl.ds(0, (2 * nx - 1) * rows)], wrecv.at[u])

        for layer in range(2):
            kind = H1 if layer == 0 else H2
            ag_src[kind] = jnp.where(keep, state[layer], 0.0).astype(BF16)
            to_all(kind)
            to_blocks(layer, layer)

        def copy_row_block():
            blk[:, column_slice(x)] = ag_src[H2]
            for k, (dx, dy) in enumerate(offsets):
                if dy == 0:
                    blk[:, column_slice(wrap(x - dx, nx))] = ag_buf[H2, k]

        def reset_phase(layer, kind, unit, slot, buf, sem):
            wait_in(buf.at[0], sem)
            pre = gathered_dot(kind, unit, partial_sum(buf, slot, 0) + bias[layer, 0:1])
            if layer == 1:
                copy_row_block()
            gate = jax.nn.sigmoid(pre)
            out = RH1 if layer == 0 else RH2
            ag_src[out] = jnp.where(keep, gate * state[layer], 0.0).astype(BF16)
            to_all(out)
            sent(kind)
            sent_blocks(layer)

        def candidate_phase(layer, unit, slot, buf, ubuf, usem):
            kind = RH1 if layer == 0 else RH2
            pre = gathered_dot(kind, unit, partial_sum(buf, slot, 1) + bias[layer, 2:3])
            cand = jnp.tanh(pre)
            wait_in(ubuf.at[0], usem)
            upd = jax.nn.sigmoid(partial_sum(ubuf, slot, 0) + bias[layer, 1:2])
            new = (1.0 - upd) * cand + upd * state[layer]
            state[layer] = new
            return jnp.where(keep, new, 0.0).astype(BF16)

        part = block // (2 * nx)

        def step(i, carry):
            @pl.when(i < steps)
            def _():
                @pl.when(i == 0)
                def _():
                    wait_weights(R1)
                slot = lax.rem(i, RING)
                reset_phase(0, H1, R1, slot, p_x, rs_recv.at[1, slot])

            @pl.when(i >= 2)
            def _():
                t = i - 2
                slot = lax.rem(t, RING)

                @pl.when(i == 2)
                def _():
                    wait_weights(N2)
                new = candidate_phase(1, N2, slot, p_p, p_u2, rs_recv.at[3, slot])
                sent(RH2)

                @pl.when(t < steps - 1)
                def _():
                    ag_src[H2] = new
                    to_all(H2)
                    to_blocks(1, lax.rem(t, 2))

            @pl.when(i < steps)
            def _():
                @pl.when(i == 0)
                def _():
                    wait_weights(N1)
                slot = lax.rem(i, RING)
                new = candidate_phase(0, N1, slot, p_x, p_u1, rs_recv.at[0, slot])
                sent(RH1)
                ag_src[H1] = new

                @pl.when(i < steps - 1)
                def _():
                    to_all(H1)
                to_blocks(0, lax.rem(i + 1, 2))

            @pl.when(jnp.logical_and(i >= 1, i < steps + 1))
            def _():
                @pl.when(i == 1)
                def _():
                    wait_weights(R2)
                slot = lax.rem(i - 1, RING)
                reset_phase(1, H2, R2, slot, p_p, rs_recv.at[2, slot])

                @pl.when(i >= 2)
                def _():
                    for k in range(nx):
                        @pl.when(x == k)
                        def _():
                            out_s[i - 2] = blk[:, 2 * k * part:(2 * k + 1) * part]
                            out_n[i - 2] = blk[:, (2 * k + 1) * part:(2 * k + 2) * part]
            return carry

        lax.fori_loop(0, steps + 2, step, 0)
        sent_blocks(0)

        fin_src[...] = state[...]
        for d in range(1, nx):
            tx = wrap(x + d, nx)
            remote(fin_src, fin_buf.at[d], f_sem.at[0], f_sem.at[1], tx, 1, y).start()
        fblk[:, :, column_slice(x)] = state[...]
        wait_in(fin_buf.at[pl.ds(1, nx - 1)], f_sem.at[1])
        for d in range(1, nx):
            fblk[:, :, column_slice(wrap(x - d, nx))] = fin_buf[d]
        for k in range(nx):
            @pl.when(x == k)
            def _():
                s_part = fblk[:, :, 2 * k * part:(2 * k + 1) * part]
                n_part = fblk[:, :, (2 * k + 1) * part:(2 * k + 2) * part]
                fin_s[...] = s_part
                fin_n[...] = n_part
                out_s[steps - 1] = s_part[1].astype(BF16)
                out_n[steps - 1] = n_part[1].astype(BF16)
        remote(fin_s, fin_s, o_sem.at[2], o_sem.at[3], x, 0, y).start()
        remote(out_s, out_s, o_sem.at[0], o_sem.at[1], x, 0, y).start()
        seq_out[...] = out_n[...]
        fin_out[...] = fin_n[...]
        wait_in(fin_s, o_sem.at[2])
        wait_in(out_s, o_sem.at[0])
        wait_in(fin_buf.at[pl.ds(1, nx - 1)], f_sem.at[0])
        wait_in(xb.at[1], x_sem.at[0])
        for u in range(4):
            wait_in(w_own.at[0, pl.ds(0, (nx - 1) * rows)], wsend.at[u])
        for u in range(8):
            wait_in(w_blk.at[0, pl.ds(rows, rows)], bs_send.at[u])


def solution(mesh):
    nx, ny = mesh.shape["row"] // 2, mesh.shape["col"]
    seq_spec = P(None, "data", "row")
    out_spec = P(None, "data", ("col", "row"))
    wide_spec = P("row", None, "col")
    square_spec = P("row", "col")
    bias_spec = P(None, "col")

    def device_body(x_rows, h_rows, wx_l1, whru_l1, whn_l1, bias_l1, wx_l2, whru_l2, whn_l2, bias_l2):
        steps, batch, rows = x_rows.shape
        cols = whn_l1.shape[1]
        chunk = cdiv(cdiv(cols, nx), LANES) * LANES
        wide = nx * chunk
        part = cols // (2 * nx)
        dims = (steps, batch, rows, cols, nx, ny, chunk)

        def padded(w):
            return jnp.pad(w, ((0, 0), (0, wide - cols)))

        peers = nx * ny - 1
        total_rows = nx * cols
        hbm = pl.BlockSpec(memory_space=pl.ANY)
        vmem = pl.BlockSpec(memory_space=pltpu.VMEM)
        dma = pltpu.SemaphoreType.DMA
        operands = []
        specs = []
        for lead, wx, wru, wn, b in (((x_rows, h_rows), wx_l1, whru_l1, whn_l1, bias_l1), ((), wx_l2, whru_l2, whn_l2, bias_l2)):
            if lead:
                operands += list(lead)
                specs += [hbm, vmem]
            operands += [jnp.transpose(wx, (1, 0, 2)), wru[:, 1], padded(wru[:, 0]), padded(wn), b]
            specs += [hbm, hbm, hbm, hbm, vmem]
        scratch = [
            pltpu.VMEM((4, total_rows + wide - cols, chunk), BF16),
            pltpu.VMEM((8, 2 * rows, cols), BF16),
            pltpu.VMEM((2, steps, batch, rows), BF16),
            pltpu.VMEM((2, batch, wide), F32),
            pltpu.VMEM((2, batch, rows), F32),
            pltpu.VMEM((2, batch, chunk), F32),
            pltpu.VMEM((4, batch, chunk), BF16),
            pltpu.VMEM((4, peers, batch, chunk), BF16),
            pltpu.VMEM((2, 2, batch, wide), BF16),
            pltpu.VMEM((2, 8, chunk), F32),
            pltpu.VMEM((2, 8, wide), F32),
            pltpu.VMEM((RING, nx, 1, batch, chunk), F32),
            pltpu.VMEM((RING, nx, 2, batch, chunk), F32),
            pltpu.VMEM((RING, nx, 2, batch, chunk), F32),
            pltpu.VMEM((RING, nx, 1, batch, chunk), F32),
            pltpu.VMEM((1, batch, wide), F32),
            pltpu.VMEM((2, batch, wide), F32),
            pltpu.VMEM((2, batch, wide), F32),
            pltpu.VMEM((1, batch, wide), F32),
            pltpu.VMEM((batch, cols), F32),
            pltpu.VMEM((batch, cols), F32),
            pltpu.VMEM((batch, wide), BF16),
            pltpu.VMEM((steps, batch, part), BF16),
            pltpu.VMEM((steps, batch, part), BF16),
            pltpu.VMEM((2, batch, chunk), F32),
            pltpu.VMEM((nx, 2, batch, chunk), F32),
            pltpu.VMEM((2, batch, wide), F32),
            pltpu.VMEM((2, batch, part), F32),
            pltpu.VMEM((2, batch, part), F32),
            dma((8,)),
            dma((4,)),
            dma((4,)),
            dma((4,)),
            dma((8,)),
            dma((8,)),
            dma((2,)),
            dma((4,)),
            dma((4,)),
            dma((4, 4)),
            dma((2,)),
            dma((2, 2)),
            dma((4,)),
            dma((4, RING)),
            dma((2,)),
            dma((4,)),
        ]
        return pl.pallas_call(
            functools.partial(gru_kernel, dims),
            name="gru",
            out_shape=(
                jax.ShapeDtypeStruct((steps, batch, part), BF16),
                jax.ShapeDtypeStruct((2, batch, part), F32),
            ),
            in_specs=specs,
            out_specs=(vmem, vmem),
            scratch_shapes=scratch,
            compiler_params=pltpu.CompilerParams(
                collective_id=0, has_side_effects=True, vmem_limit_bytes=61 * 1024 * 1024
            ),
        )(*operands)

    return jax.shard_map(
        device_body,
        mesh=mesh,
        in_specs=(seq_spec, seq_spec, wide_spec, wide_spec, square_spec, bias_spec, wide_spec, wide_spec, square_spec, bias_spec),
        out_specs=(out_spec, out_spec),
        check_vma=False,
    )
```

```python
import functools

import jax
import jax.numpy as jnp
from jax import lax
from jax.experimental import pallas as pl
from jax.experimental.pallas import tpu as pltpu
from jax.sharding import PartitionSpec as P

MESH = pl.DeviceIdType.MESH
F32 = jnp.float32
BF16 = jnp.bfloat16
LANES = 128

H1, H2, RH1, RH2 = 0, 2, 4, 5
R1, N1, R2, N2 = range(4)
XR, XU, XN, PR, PU, PN, U1, U2 = range(8)
RING = 4


def cdiv(a, b):
    return -(-a // b)


def hop(d, n):
    return min(d, n - d)


def nx_hops(nx, ny):
    return [hop(dx, nx) + hop(dy, ny) for dx in range(nx) for dy in range(ny) if (dx, dy) != (0, 0)]


def gru_kernel(dims, *refs):
    steps, batch, rows, cols, nx, ny, chunk = dims
    (x_hbm, h0, wx1, wru1, wn1, b1, wx2, wru2, wn2, b2,
     seq_out, fin_out,
     w_own, w_blk, w_upd, xb, hcat, h0s, state, ag_buf, hs, bias, bpad,
     p_u1, p_x, p_p, p_u2, s_u1, s_x, s_p, s_u2, xu_keep, pu_keep,
     blk, out_n, out_s, fin_src, fin_buf, fblk, fin_n, fin_s,
     ld_sem, wl_sem, wsend, wrecv, bs_send, bs_recv, x_sem, i_sem,
     ag_send, ag_recv, hs_send, hs_recv, rs_send, rs_recv, f_sem, o_sem) = refs
    block = 2 * rows
    device_row = lax.axis_index("row")
    y = lax.axis_index("col")
    x = device_row // 2
    core = lax.rem(device_row, 2)

    def wrap(v, n):
        return lax.rem(v + n, n)

    def remote(src, dst, ssem, rsem, tx, tc, ty):
        return pltpu.make_async_remote_copy(
            src_ref=src, dst_ref=dst, send_sem=ssem, recv_sem=rsem,
            device_id={"row": tx * 2 + tc, "col": ty}, device_id_type=MESH,
        )

    def wait_in(dst, sem):
        pltpu.make_async_copy(dst, dst, sem).wait()

    offsets = [(dx, dy) for dx in range(nx) for dy in range(ny) if (dx, dy) != (0, 0)]
    offsets.sort(key=lambda o: hop(o[0], nx) + hop(o[1], ny))
    dists = [hop(dx, nx) + hop(dy, ny) for dx, dy in offsets]
    groups = []
    for d in sorted(set(dists)):
        first = dists.index(d)
        groups.append((first, first + dists.count(d)))
    peers = len(offsets)

    barrier = pltpu.get_barrier_semaphore()
    for d in range(1, 2 * nx * ny):
        tr = lax.rem(device_row + d % (2 * nx), 2 * nx)
        ty = lax.rem(y + d // (2 * nx), ny)
        pl.semaphore_signal(barrier, inc=1, device_id={"row": tr, "col": ty}, device_id_type=MESH)

    moved = ((wru1.at[0], R1), (wn1, N1), (wru2.at[0], R2), (wn2, N2))
    kept = ((wx1.at[0], XR), (wx1.at[2], XN), (wx1.at[1], XU), (wru1.at[1], U1),
            (wx2.at[0], PR), (wx2.at[2], PN), (wx2.at[1], PU), (wru2.at[1], U2))

    def block_weight(u):
        return w_blk.at[u] if u < U1 else w_upd.at[u - U1]

    my_rows = pl.ds(pl.multiple_of(device_row * rows, 16), rows)

    def column_slice(i):
        return pl.ds(pl.multiple_of(i * chunk, LANES), chunk)

    @pl.when(core == 0)
    def _():
        loads = []
        for src, u in kept:
            loads.append(pltpu.make_async_copy(src, block_weight(u).at[pl.ds(0, rows)], ld_sem.at[u]))
        xload = pltpu.make_async_copy(x_hbm, xb.at[0], x_sem.at[0])
        xload.start()
        for c in loads:
            c.start()
        pl.semaphore_wait(barrier, 2 * nx * ny - 1)

        @pl.when(x == y)
        def _():
            remote(h0, h0s, i_sem.at[0], i_sem.at[1], x, 1, y).start()

        for src, u in moved:
            for d in range(nx):
                tx = wrap(x + d, nx)
                remote(src.at[:, column_slice(tx)], w_own.at[u, my_rows], wsend.at[u], wrecv.at[u], tx, 1, y).start()

        xload.wait()
        wait_in(xb.at[1], x_sem.at[1])

        def wait_kept(n):
            loads[n].wait()
            u = kept[n][1]
            wait_in(block_weight(u).at[pl.ds(rows, rows)], bs_recv.at[u])

        def row_dot(vec, u):
            return jnp.dot(vec, block_weight(u)[:, 0:block], preferred_element_type=F32)

        near_last = sorted(range(nx), key=lambda d: -hop(d, nx))

        def spread(src, dst, kind, slot):
            for d in near_last:
                tx = wrap(x + d, nx)
                remote(src.at[:, :, column_slice(tx)], dst.at[slot, x], rs_send.at[kind], rs_recv.at[kind, slot], tx, 1, y).start()

        def update_part(vec, u, kept_sum, kept_slot, src, dst, kind, slot):
            for d in near_last:
                tx = wrap(x + d, nx)
                src[0, :, column_slice(tx)] = (
                    jnp.dot(vec, block_weight(u)[:, column_slice(tx)], preferred_element_type=F32)
                    + kept_sum[kept_slot, :, column_slice(tx)])
                remote(src.at[:, :, column_slice(tx)], dst.at[slot, x], rs_send.at[kind], rs_recv.at[kind, slot], tx, 1, y).start()

        def spread_wait(src, kind):
            wait_in(src, rs_send.at[kind])

        def project(t):
            def half(g):
                return (jnp.dot(xb[0, t], w_blk[g, 0:rows], preferred_element_type=F32)
                        + jnp.dot(xb[1, t], w_blk[g, rows:block], preferred_element_type=F32))
            s_x[0, :, 0:block] = half(XR)
            s_x[1, :, 0:block] = half(XN)
            spread(s_x, p_x, 1, lax.rem(t, RING))
            xu_keep[lax.rem(t, 2), :, 0:block] = half(XU)

        s_u1[...] = jnp.zeros_like(s_u1)
        s_u2[...] = jnp.zeros_like(s_u2)
        s_x[...] = jnp.zeros_like(s_x)
        s_p[...] = jnp.zeros_like(s_p)
        xu_keep[...] = jnp.zeros_like(xu_keep)
        pu_keep[...] = jnp.zeros_like(pu_keep)
        for n in range(3):
            wait_kept(n)
        project(0)
        spread_wait(s_x, 1)
        project(1)
        for n in range(3, 8):
            wait_kept(n)

        def step(i, carry):
            @pl.when(i <= steps)
            def _():
                wait_in(hs.at[0, 0], hs_recv.at[0, lax.rem(i, RING)])

            @pl.when(i < steps)
            def _():
                @pl.when(i > 0)
                def _():
                    spread_wait(s_u1, 0)
                update_part(hs[0, lax.rem(i, RING), :, 0:block], U1, xu_keep, lax.rem(i, 2), s_u1, p_u1, 0, lax.rem(i, RING))

            @pl.when(jnp.logical_and(i >= 1, i <= steps))
            def _():
                h1v = hs[0, lax.rem(i, RING), :, 0:block]

                @pl.when(i > 1)
                def _():
                    spread_wait(s_p, 2)
                s_p[0, :, 0:block] = row_dot(h1v, PR)
                s_p[1, :, 0:block] = row_dot(h1v, PN)
                spread(s_p, p_p, 2, lax.rem(i + 3, RING))
                pu_keep[lax.rem(i + 1, 2), :, 0:block] = row_dot(h1v, PU)

            @pl.when(i >= 2)
            def _():
                wait_in(hs.at[1, 0], hs_recv.at[1, lax.rem(i, RING)])

                @pl.when(i > 2)
                def _():
                    spread_wait(s_u2, 3)
                update_part(hs[1, lax.rem(i, RING), :, 0:block], U2, pu_keep, lax.rem(i, 2), s_u2, p_u2, 3, lax.rem(i + 2, RING))

            @pl.when(i + 2 < steps)
            def _():
                spread_wait(s_x, 1)
                project(i + 2)
            return carry

        lax.fori_loop(0, steps + 2, step, 0)
        spread_wait(s_u1, 0)
        spread_wait(s_x, 1)
        spread_wait(s_p, 2)
        spread_wait(s_u2, 3)
        for u in range(4):
            wait_in(w_own.at[0, pl.ds(0, nx * rows)], wsend.at[u])

        @pl.when(x == y)
        def _():
            wait_in(h0, i_sem.at[0])
        wait_in(out_s, o_sem.at[1])
        wait_in(fin_s, o_sem.at[3])
        seq_out[...] = out_s[...]
        fin_out[...] = fin_s[...]

    @pl.when(core == 1)
    def _():
        own = []
        for src, u in moved:
            own.append(pltpu.make_async_copy(src.at[:, column_slice(x)], w_own.at[u, my_rows], wl_sem.at[u]))
        for c in own:
            c.start()
        pl.semaphore_wait(barrier, 2 * nx * ny - 1)

        def move(src, u):
            for d in range(1, nx):
                tx = wrap(x + d, nx)
                remote(src.at[:, column_slice(tx)], w_own.at[u, my_rows], wsend.at[u], wrecv.at[u], tx, 1, y).start()

        move(*moved[0])
        remote(x_hbm, xb.at[1], x_sem.at[0], x_sem.at[1], x, 0, y).start()
        for src, u in kept:
            remote(src, block_weight(u).at[pl.ds(rows, rows)], bs_send.at[u], bs_recv.at[u], x, 0, y).start()

        for u in range(4):
            w_own[u, pl.ds(nx * block, chunk * nx - block)] = jnp.zeros((chunk * nx - block, chunk), BF16)
        bpad[...] = jnp.zeros_like(bpad)
        bpad[0, 0:3, 0:block] = b1[...]
        bpad[1, 0:3, 0:block] = b2[...]
        bias[...] = bpad[:, :, column_slice(x)]
        valid = jnp.minimum(block - x * chunk, chunk)
        keep = lax.broadcasted_iota(jnp.int32, (batch, chunk), 1) < valid

        @pl.when(x == y)
        def _():
            wait_in(h0s, i_sem.at[1])
            hcat[...] = jnp.zeros_like(hcat)
            hcat[:, :, 0:rows] = h0s[...]
            hcat[:, :, rows:block] = h0[...]
            for d in range(1, nx):
                tx = wrap(x + d, nx)
                remote(hcat.at[:, :, column_slice(tx)], state, i_sem.at[2], i_sem.at[3], tx, 1, y).start()
            state[...] = hcat[:, :, column_slice(x)]
            wait_in(hcat.at[:, :, pl.ds(0, (nx - 1) * chunk)], i_sem.at[2])

        @pl.when(x != y)
        def _():
            wait_in(state, i_sem.at[3])

        def to_all(kind):
            for k in reversed(range(peers)):
                dx, dy = offsets[k]
                g = [j for j, (a, b) in enumerate(groups) if a <= k < b][0]
                remote(ag_buf.at[kind, 0, 0], ag_buf.at[kind, dy, dx], ag_send.at[kind], ag_recv.at[kind, g],
                       wrap(x + dx, nx), 1, wrap(y + dy, ny)).start()

        def to_block(layer, kind, slot):
            dy = wrap(y - x, ny)
            for dx in range(nx):
                remote(ag_buf.at[kind, dy, dx], hs.at[layer, slot, :, column_slice(wrap(x - dx, nx))],
                       hs_send.at[layer], hs_recv.at[layer, slot], x, 0, y).start()

        def chunks(n):
            return w_own.at[0, pl.ds(0, n * batch)]

        def sent(kind):
            wait_in(chunks(peers), ag_send.at[kind])

        def sent_blocks(layer):
            wait_in(chunks(nx), hs_send.at[layer])

        def weight_rows(dx, dy):
            sx, sy = wrap(x - dx, nx), wrap(y - dy, ny)
            return pl.ds(pl.multiple_of(sy * block + sx * chunk, 32), chunk)

        def arrive(kind, g):
            a, b = groups[g]
            wait_in(chunks(b - a), ag_recv.at[kind, g])

        def gathered_dot(kind, u, acc):
            acc = acc + jnp.dot(ag_buf[kind, 0, 0], w_own[u, weight_rows(0, 0)], preferred_element_type=F32)
            for g, (a, b) in enumerate(groups):
                arrive(kind, g)
                for dx, dy in offsets[a:b]:
                    acc = acc + jnp.dot(ag_buf[kind, dy, dx], w_own[u, weight_rows(dx, dy)], preferred_element_type=F32)
            return acc

        def partial_sum(buf, slot, g):
            total = buf[slot, 0, g]
            for s in range(1, nx):
                total = total + buf[slot, s, g]
            return total

        def wait_weights(u):
            own[u].wait()
            wait_in(w_own.at[u, pl.ds(0, (2 * nx - 1) * rows)], wrecv.at[u])

        for layer in range(2):
            kind = H1 if layer == 0 else H2
            ag_buf[kind, 0, 0] = jnp.where(keep, state[layer], 0.0).astype(BF16)
            to_all(kind)
        for src, u in moved[1:]:
            move(src, u)

        def copy_row_block(kind):
            blk[:, column_slice(x)] = ag_buf[kind, 0, 0]
            for dx in range(1, nx):
                blk[:, column_slice(wrap(x - dx, nx))] = ag_buf[kind, 0, dx]

        def reset_phase(layer, kind, unit, slot, buf, sem, hslot):
            wait_in(buf.at[0], sem)
            pre = gathered_dot(kind, unit, partial_sum(buf, slot, 0) + bias[layer, 0:1])
            to_block(layer, kind, hslot)
            if layer == 1:
                copy_row_block(kind)
            gate = jax.nn.sigmoid(pre)
            out = RH1 if layer == 0 else RH2
            ag_buf[out, 0, 0] = jnp.where(keep, gate * state[layer], 0.0).astype(BF16)
            to_all(out)
            sent(kind)

        def candidate_phase(layer, unit, slot, buf, ubuf, usem):
            kind = RH1 if layer == 0 else RH2
            pre = gathered_dot(kind, unit, partial_sum(buf, slot, 1) + bias[layer, 2:3])
            cand = jnp.tanh(pre)
            wait_in(ubuf.at[0], usem)
            upd = jax.nn.sigmoid(partial_sum(ubuf, slot, 0) + bias[layer, 1:2])
            new = (1.0 - upd) * cand + upd * state[layer]
            state[layer] = new
            return jnp.where(keep, new, 0.0).astype(BF16)

        part = block // (2 * nx)

        def step(i, carry):
            slot1 = lax.rem(i, RING)
            t2 = i - 2
            slot2 = lax.rem(i + 2, RING)

            @pl.when(i < steps)
            def _():
                @pl.when(i == 0)
                def _():
                    wait_weights(R1)
                reset_phase(0, H1 + lax.rem(i, 2), R1, slot1, p_x, rs_recv.at[1, slot1], slot1)

            @pl.when(i == steps)
            def _():
                kind = H1 + lax.rem(i, 2)
                for g in range(len(groups)):
                    arrive(kind, g)
                to_block(0, kind, slot1)
                sent(kind)

            @pl.when(t2 >= 0)
            def _():
                @pl.when(t2 == 0)
                def _():
                    wait_weights(R2)
                reset_phase(1, H2 + lax.rem(i, 2), R2, slot2, p_p, rs_recv.at[2, slot2], slot1)

                @pl.when(t2 >= 1)
                def _():
                    for k in range(nx):
                        @pl.when(x == k)
                        def _():
                            out_s[t2 - 1] = blk[:, 2 * k * part:(2 * k + 1) * part]
                            out_n[t2 - 1] = blk[:, (2 * k + 1) * part:(2 * k + 2) * part]

            @pl.when(i < steps)
            def _():
                @pl.when(i == 0)
                def _():
                    wait_weights(N1)
                new = candidate_phase(0, N1, slot1, p_x, p_u1, rs_recv.at[0, slot1])
                ag_buf[H1 + lax.rem(i + 1, 2), 0, 0] = new
                to_all(H1 + lax.rem(i + 1, 2))
                sent(RH1)
                sent_blocks(0)

            @pl.when(t2 >= 0)
            def _():
                @pl.when(t2 == 0)
                def _():
                    wait_weights(N2)
                new = candidate_phase(1, N2, slot2, p_p, p_u2, rs_recv.at[3, slot2])

                @pl.when(t2 < steps - 1)
                def _():
                    ag_buf[H2 + lax.rem(i + 1, 2), 0, 0] = new
                    to_all(H2 + lax.rem(i + 1, 2))
                sent(RH2)
                sent_blocks(1)
            return carry

        lax.fori_loop(0, steps + 2, step, 0)
        sent_blocks(0)

        fin_src[...] = state[...]
        for d in range(1, nx):
            tx = wrap(x + d, nx)
            remote(fin_src, fin_buf.at[d], f_sem.at[0], f_sem.at[1], tx, 1, y).start()
        fblk[:, :, column_slice(x)] = state[...]
        wait_in(fin_buf.at[pl.ds(1, nx - 1)], f_sem.at[1])
        for d in range(1, nx):
            fblk[:, :, column_slice(wrap(x - d, nx))] = fin_buf[d]
        for k in range(nx):
            @pl.when(x == k)
            def _():
                s_part = fblk[:, :, 2 * k * part:(2 * k + 1) * part]
                n_part = fblk[:, :, (2 * k + 1) * part:(2 * k + 2) * part]
                fin_s[...] = s_part
                fin_n[...] = n_part
                out_s[steps - 1] = s_part[1].astype(BF16)
                out_n[steps - 1] = n_part[1].astype(BF16)
        remote(fin_s, fin_s, o_sem.at[2], o_sem.at[3], x, 0, y).start()
        remote(out_s, out_s, o_sem.at[0], o_sem.at[1], x, 0, y).start()
        seq_out[...] = out_n[...]
        fin_out[...] = fin_n[...]
        wait_in(fin_s, o_sem.at[2])
        wait_in(out_s, o_sem.at[0])
        wait_in(fin_buf.at[pl.ds(1, nx - 1)], f_sem.at[0])
        wait_in(xb.at[1], x_sem.at[0])
        for u in range(4):
            wait_in(w_own.at[0, pl.ds(0, (nx - 1) * rows)], wsend.at[u])
        for u in range(8):
            wait_in(block_weight(u).at[pl.ds(rows, rows)], bs_send.at[u])


def solution(mesh):
    nx, ny = mesh.shape["row"] // 2, mesh.shape["col"]
    seq_spec = P(None, "data", "row")
    out_spec = P(None, "data", ("col", "row"))
    wide_spec = P("row", None, "col")
    square_spec = P("row", "col")
    bias_spec = P(None, "col")

    def device_body(x_rows, h_rows, wx_l1, whru_l1, whn_l1, bias_l1, wx_l2, whru_l2, whn_l2, bias_l2):
        steps, batch, rows = x_rows.shape
        cols = whn_l1.shape[1]
        chunk = cdiv(cdiv(cols, nx), LANES) * LANES
        wide = nx * chunk
        part = cols // (2 * nx)
        dims = (steps, batch, rows, cols, nx, ny, chunk)

        peers = nx * ny - 1
        total_rows = nx * cols
        hbm = pl.BlockSpec(memory_space=pl.ANY)
        vmem = pl.BlockSpec(memory_space=pltpu.VMEM)
        dma = pltpu.SemaphoreType.DMA
        operands = []
        specs = []
        for lead, wx, wru, wn, b in (((x_rows, h_rows), wx_l1, whru_l1, whn_l1, bias_l1), ((), wx_l2, whru_l2, whn_l2, bias_l2)):
            if lead:
                operands += list(lead)
                specs += [hbm, vmem]
            wru = jnp.pad(jnp.transpose(wru, (1, 0, 2)), ((0, 0), (0, 0), (0, wide - cols)))
            operands += [jnp.transpose(wx, (1, 0, 2)), wru, jnp.pad(wn, ((0, 0), (0, wide - cols))), b]
            specs += [hbm, hbm, hbm, vmem]
        scratch = [
            pltpu.VMEM((4, total_rows + wide - cols, chunk), BF16),
            pltpu.VMEM((6, 2 * rows, cols), BF16),
            pltpu.VMEM((2, 2 * rows, wide), BF16),
            pltpu.VMEM((2, steps, batch, rows), BF16),
            pltpu.VMEM((2, batch, wide), F32),
            pltpu.VMEM((2, batch, rows), F32),
            pltpu.VMEM((2, batch, chunk), F32),
            pltpu.VMEM((6, ny, nx, batch, chunk), BF16),
            pltpu.VMEM((2, RING, batch, wide), BF16),
            pltpu.VMEM((2, 8, chunk), F32),
            pltpu.VMEM((2, 8, wide), F32),
            pltpu.VMEM((RING, nx, 1, batch, chunk), F32),
            pltpu.VMEM((RING, nx, 2, batch, chunk), F32),
            pltpu.VMEM((RING, nx, 2, batch, chunk), F32),
            pltpu.VMEM((RING, nx, 1, batch, chunk), F32),
            pltpu.VMEM((1, batch, wide), F32),
            pltpu.VMEM((2, batch, wide), F32),
            pltpu.VMEM((2, batch, wide), F32),
            pltpu.VMEM((1, batch, wide), F32),
            pltpu.VMEM((2, batch, wide), F32),
            pltpu.VMEM((2, batch, wide), F32),
            pltpu.VMEM((batch, wide), BF16),
            pltpu.VMEM((steps, batch, part), BF16),
            pltpu.VMEM((steps, batch, part), BF16),
            pltpu.VMEM((2, batch, chunk), F32),
            pltpu.VMEM((nx, 2, batch, chunk), F32),
            pltpu.VMEM((2, batch, wide), F32),
            pltpu.VMEM((2, batch, part), F32),
            pltpu.VMEM((2, batch, part), F32),
            dma((8,)),
            dma((4,)),
            dma((4,)),
            dma((4,)),
            dma((8,)),
            dma((8,)),
            dma((2,)),
            dma((4,)),
            dma((6,)),
            dma((6, len(set(nx_hops(nx, ny))))),
            dma((2,)),
            dma((2, RING)),
            dma((4,)),
            dma((4, RING)),
            dma((2,)),
            dma((4,)),
        ]
        return pl.pallas_call(
            functools.partial(gru_kernel, dims),
            name="gru",
            out_shape=(
                jax.ShapeDtypeStruct((steps, batch, part), BF16),
                jax.ShapeDtypeStruct((2, batch, part), F32),
            ),
            in_specs=specs,
            out_specs=(vmem, vmem),
            scratch_shapes=scratch,
            compiler_params=pltpu.CompilerParams(
                collective_id=0, has_side_effects=True, vmem_limit_bytes=61 * 1024 * 1024
            ),
        )(*operands)

    return jax.shard_map(
        device_body,
        mesh=mesh,
        in_specs=(seq_spec, seq_spec, wide_spec, wide_spec, square_spec, bias_spec, wide_spec, wide_spec, square_spec, bias_spec),
        out_specs=(out_spec, out_spec),
        check_vma=False,
    )
```

```python
import functools

import jax
import jax.numpy as jnp
from jax import lax
from jax.experimental import pallas as pl
from jax.experimental.pallas import tpu as pltpu
from jax.sharding import PartitionSpec as P

MESH = pl.DeviceIdType.MESH
F32 = jnp.float32
BF16 = jnp.bfloat16
LANES = 128
TILE = 256

STATE, GATED = range(2)
RESET, CAND = range(2)
XR, XU, XN, PR, PU, PN, U1, U2 = range(8)
K_U1, K_X, K_P, K_U2 = range(4)
RING = 4


def hop(d, n):
    return min(d, n - d)


def gru_kernel(dims, *refs):
    steps, batch, rows, nx, ny, chunk = dims
    (x_hbm, h0, wx1, wru1, wn1, b1, wx2, wru2, wn2, b2,
     seq_out, fin_out,
     w_own, w_blk, w_upd, xb, hcat, h0s, state, ag_buf, hs, bias, bpad,
     p_in, p_upd, s_u1, s_x, s_p, s_u2, xu_keep, pu_keep,
     blk, out_own, out_s, out_far, fin_buf, fblk, fin_n, fin_s, last_s,
     ld_sem, wl_sem, wsend, wrecv, bs_send, bs_recv, x_sem, i_sem,
     ag_send, ag_recv, hs_send, hs_recv, rs_send, in_recv, upd_recv, f_sem, o_send, o_recv, d_sem) = refs
    block = 2 * rows
    half = nx // 2
    part = block // (2 * nx)
    device_row = lax.axis_index("row")
    y = lax.axis_index("col")
    x = device_row // 2
    core = lax.rem(device_row, 2)

    def wrap(v, n):
        return lax.rem(v + n, n)

    def remote(src, dst, ssem, rsem, tx, tc, ty):
        return pltpu.make_async_remote_copy(
            src_ref=src, dst_ref=dst, send_sem=ssem, recv_sem=rsem,
            device_id={"row": tx * 2 + tc, "col": ty}, device_id_type=MESH,
        )

    def wait_in(dst, sem):
        pltpu.make_async_copy(dst, dst, sem).wait()

    def column_slice(i):
        return pl.ds(pl.multiple_of(i * chunk, LANES), chunk)

    barrier = pltpu.get_barrier_semaphore()
    for d in range(1, 2 * nx * ny):
        tr = lax.rem(device_row + d % (2 * nx), 2 * nx)
        ty = lax.rem(y + d // (2 * nx), ny)
        pl.semaphore_signal(barrier, inc=1, device_id={"row": tr, "col": ty}, device_id_type=MESH)

    moved = {RESET: (wru1.at[0], wru2.at[0]), CAND: (wn1, wn2)}
    kept = ((wx1.at[0], XR), (wx1.at[2], XN), (wx1.at[1], XU), (wru1.at[1], U1),
            (wx2.at[0], PR), (wx2.at[2], PN), (wx2.at[1], PU), (wru2.at[1], U2))
    my_rows = pl.ds(pl.multiple_of(device_row * rows, 16), rows)

    def block_weight(u):
        return w_blk.at[u] if u < U1 else w_upd.at[u - U1]

    def move(u, offsets):
        for d in offsets:
            tx = wrap(x + d, nx)
            for layer in range(2):
                @pl.when(tx // half == layer)
                def _():
                    remote(moved[u][layer].at[:, column_slice(lax.rem(tx, half))], w_own.at[u, my_rows],
                           wsend.at[u], wrecv.at[u], tx, 1, y).start()

    @pl.when(core == 0)
    def _():
        loads = []
        for src, u in kept:
            loads.append(pltpu.make_async_copy(src, block_weight(u).at[pl.ds(0, rows)], ld_sem.at[u]))
        xload = pltpu.make_async_copy(x_hbm, xb.at[0], x_sem.at[0])
        xload.start()
        for c in loads:
            c.start()
        pl.semaphore_wait(barrier, 2 * nx * ny - 1)

        @pl.when(x == y)
        def _():
            remote(h0, h0s, i_sem.at[0], i_sem.at[1], x, 1, y).start()

        move(RESET, range(nx))
        for ref in (s_u1, s_u2, s_x, s_p, xu_keep, pu_keep):
            ref[...] = jnp.zeros_like(ref)
        xload.wait()
        wait_in(xb.at[1], x_sem.at[1])

        def wait_kept(n):
            loads[n].wait()
            u = kept[n][1]
            wait_in(block_weight(u).at[pl.ds(rows, rows)], bs_recv.at[u])

        def row_dot(vec, u):
            return jnp.dot(vec, block_weight(u)[:, 0:block], preferred_element_type=F32)

        def owners(layer):
            xs = lax.rem(x, half)
            first = jnp.where(x // half == layer, lax.rem(xs + 1, half), xs)
            return [lax.rem(first + j, half) for j in range(half)]

        def send_part(src, dst, kind, layer, slot, j, rsem):
            remote(src.at[:, :, column_slice(j)], dst.at[slot, x], rs_send.at[kind], rsem.at[slot], layer * half + j, 1, y).start()

        def spread(src, kind, layer, slot):
            for j in owners(layer):
                send_part(src, p_in, kind, layer, slot, j, in_recv)

        def spread_wait(src, kind):
            wait_in(src, rs_send.at[kind])

        def update_part(vec, u, kept_sum, kept_slot, src, kind, layer, slot):
            for j in owners(layer):
                src[0, :, column_slice(j)] = (
                    jnp.dot(vec, block_weight(u)[:, column_slice(j)], preferred_element_type=F32)
                    + kept_sum[kept_slot, :, column_slice(j)])
                send_part(src, p_upd, kind, layer, slot, j, upd_recv)

        def project(t):
            def rows_of(g):
                return (jnp.dot(xb[0, t], w_blk[g, 0:rows], preferred_element_type=F32)
                        + jnp.dot(xb[1, t], w_blk[g, rows:block], preferred_element_type=F32))
            s_x[0, :, 0:block] = rows_of(XR)
            s_x[1, :, 0:block] = rows_of(XN)
            spread(s_x, K_X, 0, lax.rem(t, RING))
            xu_keep[lax.rem(t, 2), :, 0:block] = rows_of(XU)

        def state_block(layer, slot):
            return hs[layer, slot, :, 0:block]

        def first_update(i):
            update_part(state_block(0, lax.rem(i, RING)), U1, xu_keep, lax.rem(i, 2), s_u1, K_U1, 0, lax.rem(i, RING))

        for n in range(3):
            wait_kept(n)
        project(0)
        spread_wait(s_x, K_X)
        project(1)
        for n in range(3, 8):
            wait_kept(n)
        wait_in(hs.at[0, 0], hs_recv.at[0, 0])
        first_update(0)
        move(CAND, range(nx))

        def step(i, carry):
            @pl.when(jnp.logical_and(i >= 1, i <= steps))
            def _():
                wait_in(hs.at[0, 0], hs_recv.at[0, lax.rem(i, RING)])

                @pl.when(i < steps)
                def _():
                    spread_wait(s_u1, K_U1)
                    first_update(i)

                h1v = state_block(0, lax.rem(i, RING))

                @pl.when(i > 1)
                def _():
                    spread_wait(s_p, K_P)
                s_p[0, :, 0:block] = row_dot(h1v, PR)
                s_p[1, :, 0:block] = row_dot(h1v, PN)
                spread(s_p, K_P, 1, lax.rem(i + 3, RING))
                pu_keep[lax.rem(i + 1, 2), :, 0:block] = row_dot(h1v, PU)

            @pl.when(i >= 2)
            def _():
                wait_in(hs.at[1, 0], hs_recv.at[1, lax.rem(i + 2, RING)])

                @pl.when(i > 2)
                def _():
                    spread_wait(s_u2, K_U2)
                update_part(state_block(1, lax.rem(i + 2, RING)), U2, pu_keep, lax.rem(i, 2), s_u2, K_U2, 1, lax.rem(i + 2, RING))

            @pl.when(i + 2 < steps)
            def _():
                spread_wait(s_x, K_X)
                project(i + 2)
            return carry

        lax.fori_loop(0, steps + 2, step, 0)
        spread_wait(s_u1, K_U1)
        spread_wait(s_x, K_X)
        spread_wait(s_p, K_P)
        spread_wait(s_u2, K_U2)
        for u in range(2):
            wait_in(w_own.at[0, pl.ds(0, nx * rows)], wsend.at[u])

        @pl.when(x == y)
        def _():
            wait_in(h0, i_sem.at[0])
        wait_in(out_own.at[pl.ds(0, steps - 1)], o_recv)
        wait_in(fin_s, d_sem.at[1])
        wait_in(last_s, d_sem.at[3])
        seq_out[pl.ds(0, steps - 1)] = out_own[pl.ds(0, steps - 1)]
        seq_out[steps - 1] = last_s[...]
        fin_out[...] = fin_s[...]

    @pl.when(core == 1)
    def _():
        layer = x // half
        xs = lax.rem(x, half)
        other = nx - 1 - x
        for u in range(2):
            for l in range(2):
                @pl.when(layer == l)
                def _():
                    pltpu.make_async_copy(moved[u][l].at[:, column_slice(xs)], w_own.at[u, my_rows], wl_sem.at[u]).start()
        pl.semaphore_wait(barrier, 2 * nx * ny - 1)

        @pl.when(x == y)
        def _():
            wait_in(h0s, i_sem.at[1])
            hcat[...] = jnp.zeros_like(hcat)
            hcat[:, :, 0:rows] = h0s[...]
            hcat[:, :, rows:block] = h0[...]
            for d in range(1, nx):
                tx = wrap(x + d, nx)
                remote(hcat.at[tx // half, :, column_slice(lax.rem(tx, half))], state, i_sem.at[2], i_sem.at[3], tx, 1, y).start()
            state[...] = hcat[layer, :, column_slice(xs)]

        move(RESET, range(1, nx))
        remote(x_hbm, xb.at[1], x_sem.at[0], x_sem.at[1], x, 0, y).start()
        for src, u in kept:
            remote(src, block_weight(u).at[pl.ds(rows, rows)], bs_send.at[u], bs_recv.at[u], x, 0, y).start()

        offsets = [(dx, dy) for dx in range(half) for dy in range(ny) if (dx, dy) != (0, 0)]
        offsets.sort(key=lambda o: (o[0], hop(o[1], ny)))
        peers = len(offsets)
        groups = ((0, 2), (2, 4), (4, 7))
        across = [o for o in reversed(offsets) if o[0]]
        along = [o for o in reversed(offsets) if not o[0]]
        send_order = []
        while across or along:
            send_order += [q.pop(0) for q in (across, along) if q]
        pad = half * chunk - block
        for u in range(2):
            w_own[u, pl.ds(ny * block, pad)] = jnp.zeros((pad, chunk), BF16)
        bpad[...] = jnp.zeros_like(bpad)
        for l, b in enumerate((b1, b2)):
            @pl.when(layer == l)
            def _():
                bpad[0:3, 0:block] = b[...]
        bias[...] = bpad[:, column_slice(xs)]
        valid = jnp.minimum(block - xs * chunk, chunk)
        keep = lax.broadcasted_iota(jnp.int32, (batch, chunk), 1) < valid

        def to_all(kind):
            for dx, dy in send_order:
                k = offsets.index((dx, dy))
                g = [j for j, (a, b) in enumerate(groups) if a <= k < b][0]
                remote(ag_buf.at[kind, 0, 0], ag_buf.at[kind, dy, dx], ag_send.at[kind], ag_recv.at[kind, g],
                       layer * half + lax.rem(xs + dx, half), 1, wrap(y + dy, ny)).start()

        def to_blocks(slot):
            for d in sorted(range(ny), key=lambda d: -hop(d, ny)):
                remote(ag_buf.at[STATE, 0, 0], hs.at[layer, slot, :, column_slice(xs)],
                       hs_send, hs_recv.at[layer, slot], y, 0, wrap(y + d, ny)).start()

        def chunks(n):
            return w_own.at[0, pl.ds(0, n * batch)]

        def states(n):
            return p_in.at[0, pl.ds(0, n), 0]

        def weight_rows(dx, dy):
            sx, sy = wrap(xs - dx, half), wrap(y - dy, ny)
            return pl.ds(pl.multiple_of(sy * block + sx * chunk, 32), chunk)

        def arrive(kind, g):
            a, b = groups[g]
            wait_in(chunks(b - a), ag_recv.at[kind, g])

        def gathered_dot(kind, u, acc):
            cols = [acc[:, n * TILE:(n + 1) * TILE] for n in range(3)]

            def add(group):
                sums = [None] * 4
                for c, (dx, dy) in enumerate(group):
                    vec = ag_buf[kind, dy, dx]
                    for n in (0, 1, 2 + c % 2):
                        col = min(n, 2)
                        out = jnp.dot(vec, w_own[u, weight_rows(dx, dy), col * TILE:(col + 1) * TILE], preferred_element_type=F32)
                        sums[n] = out if sums[n] is None else sums[n] + out
                for n, v in enumerate(sums):
                    if v is not None:
                        cols[min(n, 2)] = cols[min(n, 2)] + v

            add([(0, 0)])
            for g, (a, b) in enumerate(groups):
                arrive(kind, g)
                add(offsets[a:b])
            return jnp.concatenate(cols, axis=1)

        def partial_sum(buf, slot, g):
            total = buf[slot, 0, g]
            for s in range(1, nx):
                total = total + buf[slot, s, g]
            return total

        def wait_weights(u):
            wait_in(w_own.at[u, pl.ds(0, rows)], wl_sem.at[u])
            wait_in(w_own.at[u, pl.ds(0, (2 * nx - 1) * rows)], wrecv.at[u])

        def take_outputs(t):
            for dx in range(half):
                blk[:, column_slice(wrap(xs - dx, half))] = ag_buf[STATE, 0, dx]
            for k in range(half, nx):
                @pl.when(x == k)
                def _():
                    o = nx - 1 - k
                    out_s[t] = blk[:, 2 * k * part:(2 * k + 1) * part]
                    out_own[t] = blk[:, (2 * k + 1) * part:(2 * k + 2) * part]
                    out_far[0, t] = blk[:, 2 * o * part:(2 * o + 1) * part]
                    out_far[1, t] = blk[:, (2 * o + 1) * part:(2 * o + 2) * part]

        done = pl.ds(0, steps - 1)

        def outputs():
            return ((out_s, 0, x), (out_far.at[0], 0, other), (out_far.at[1], 1, other))

        @pl.when(x != y)
        def _():
            wait_in(state, i_sem.at[3])
        ag_buf[STATE, 0, 0] = jnp.where(keep, state[...], 0.0).astype(BF16)
        to_blocks(0)
        to_all(STATE)
        move(CAND, range(1, nx))

        def phase(n, carry):
            t = n // 2
            p = lax.rem(n, 2)
            slot = lax.rem(t, RING)

            @pl.when(t == 0)
            def _():
                wait_weights(p)

            @pl.when(p == RESET)
            def _():
                wait_in(p_in.at[0], in_recv.at[slot])
            pre = gathered_dot(p, p, partial_sum(p_in, slot, p) + bias[pl.ds(2 * p, 1)])

            @pl.when(p == RESET)
            def _():
                @pl.when(jnp.logical_and(layer == 1, t >= 1))
                def _():
                    take_outputs(t - 1)
                gated = jax.nn.sigmoid(pre) * state[...]
                ag_buf[GATED, 0, 0] = jnp.where(keep, gated, 0.0).astype(BF16)
                to_all(GATED)
                wait_in(chunks(peers), ag_send.at[STATE])
                wait_in(chunks(ny), hs_send)

                @pl.when(jnp.logical_and(layer == 1, t == steps - 1))
                def _():
                    for n, (src, tc, tx) in enumerate(outputs()):
                        remote(src.at[done], out_own.at[done], o_send.at[n], o_recv, tx, tc, y).start()

            @pl.when(p == CAND)
            def _():
                cand = jnp.tanh(pre)
                wait_in(p_upd.at[0], upd_recv.at[slot])
                upd = jax.nn.sigmoid(partial_sum(p_upd, slot, 0) + bias[1:2])
                new = (1.0 - upd) * cand + upd * state[...]
                state[...] = new
                ag_buf[STATE, 0, 0] = jnp.where(keep, new, 0.0).astype(BF16)

                @pl.when(t < steps - 1)
                def _():
                    to_all(STATE)

                @pl.when(jnp.logical_or(layer == 0, t < steps - 1))
                def _():
                    to_blocks(lax.rem(t + 1, RING))

                wait_in(chunks(peers), ag_send.at[GATED])
            return carry

        lax.fori_loop(0, 2 * steps, phase, 0)

        for d in range(1, nx):
            tx = wrap(x + d, nx)
            remote(state, fin_buf.at[layer, xs], f_sem.at[0], f_sem.at[1], tx, 1, y).start()
        fin_buf[layer, xs] = state[...]
        wait_in(states(nx - 1), f_sem.at[1])
        for l in range(2):
            for j in range(half):
                fblk[l, :, j * chunk:(j + 1) * chunk] = fin_buf[l, j]
        for k in range(nx):
            @pl.when(x == k)
            def _():
                s_part = fblk[:, :, 2 * k * part:(2 * k + 1) * part]
                n_part = fblk[:, :, (2 * k + 1) * part:(2 * k + 2) * part]
                fin_s[...] = s_part
                fin_n[...] = n_part
                last_s[...] = s_part[1].astype(BF16)
                seq_out[steps - 1] = n_part[1].astype(BF16)
        remote(last_s, last_s, d_sem.at[2], d_sem.at[3], x, 0, y).start()
        remote(fin_s, fin_s, d_sem.at[0], d_sem.at[1], x, 0, y).start()

        @pl.when(layer == 0)
        def _():
            wait_in(out_own.at[done], o_recv)
            wait_in(chunks(ny), hs_send)

        @pl.when(layer == 1)
        def _():
            for n, (src, tc, tx) in enumerate(outputs()):
                wait_in(src.at[done], o_send.at[n])
        seq_out[done] = out_own[done]
        fin_out[...] = fin_n[...]
        wait_in(last_s, d_sem.at[2])
        wait_in(fin_s, d_sem.at[0])
        wait_in(states(nx - 1), f_sem.at[0])

        @pl.when(x == y)
        def _():
            wait_in(states(nx - 1), i_sem.at[2])
        wait_in(xb.at[1], x_sem.at[0])
        for u in range(2):
            wait_in(w_own.at[0, pl.ds(0, (nx - 1) * rows)], wsend.at[u])
        for u in range(8):
            wait_in(block_weight(u).at[pl.ds(rows, rows)], bs_send.at[u])


def solution(mesh):
    nx, ny = mesh.shape["row"] // 2, mesh.shape["col"]
    half = nx // 2
    seq_spec = P(None, "data", "row")
    out_spec = P(None, "data", ("col", "row"))
    wide_spec = P("row", None, "col")
    square_spec = P("row", "col")
    bias_spec = P(None, "col")

    def device_body(x_rows, h_rows, wx_l1, whru_l1, whn_l1, bias_l1, wx_l2, whru_l2, whn_l2, bias_l2):
        steps, batch, rows = x_rows.shape
        cols = whn_l1.shape[1]
        chunk = -(-cols // (half * LANES)) * LANES
        wide = half * chunk
        part = cols // (2 * nx)
        dims = (steps, batch, rows, nx, ny, chunk)
        groups = 1 + max(hop(dx, nx) + hop(dy, ny) for dx in range(half) for dy in range(ny))

        hbm = pl.BlockSpec(memory_space=pl.ANY)
        vmem = pl.BlockSpec(memory_space=pltpu.VMEM)
        dma = pltpu.SemaphoreType.DMA
        operands = [x_rows, h_rows]
        specs = [hbm, vmem]
        for wx, wru, wn, b in ((wx_l1, whru_l1, whn_l1, bias_l1), (wx_l2, whru_l2, whn_l2, bias_l2)):
            wru = jnp.pad(jnp.transpose(wru, (1, 0, 2)), ((0, 0), (0, 0), (0, wide - cols)))
            operands += [jnp.transpose(wx, (1, 0, 2)), wru, jnp.pad(wn, ((0, 0), (0, wide - cols))), b]
            specs += [hbm, hbm, hbm, vmem]
        scratch = [
            pltpu.VMEM((2, ny * cols + wide - cols, chunk), BF16),
            pltpu.VMEM((6, 2 * rows, cols), BF16),
            pltpu.VMEM((2, 2 * rows, wide), BF16),
            pltpu.VMEM((2, steps, batch, rows), BF16),
            pltpu.VMEM((2, batch, wide), F32),
            pltpu.VMEM((2, batch, rows), F32),
            pltpu.VMEM((batch, chunk), F32),
            pltpu.VMEM((2, ny, half, batch, chunk), BF16),
            pltpu.VMEM((2, RING, batch, wide), BF16),
            pltpu.VMEM((8, chunk), F32),
            pltpu.VMEM((8, wide), F32),
            pltpu.VMEM((RING, nx, 2, batch, chunk), F32),
            pltpu.VMEM((RING, nx, 1, batch, chunk), F32),
            pltpu.VMEM((1, batch, wide), F32),
            pltpu.VMEM((2, batch, wide), F32),
            pltpu.VMEM((2, batch, wide), F32),
            pltpu.VMEM((1, batch, wide), F32),
            pltpu.VMEM((2, batch, wide), F32),
            pltpu.VMEM((2, batch, wide), F32),
            pltpu.VMEM((batch, wide), BF16),
            pltpu.VMEM((steps, batch, part), BF16),
            pltpu.VMEM((steps, batch, part), BF16),
            pltpu.VMEM((2, steps, batch, part), BF16),
            pltpu.VMEM((2, half, batch, chunk), F32),
            pltpu.VMEM((2, batch, wide), F32),
            pltpu.VMEM((2, batch, part), F32),
            pltpu.VMEM((2, batch, part), F32),
            pltpu.VMEM((batch, part), BF16),
            dma((8,)),
            dma((2,)),
            dma((2,)),
            dma((2,)),
            dma((8,)),
            dma((8,)),
            dma((2,)),
            dma((4,)),
            dma((2,)),
            dma((2, groups)),
            dma(()),
            dma((2, RING)),
            dma((4,)),
            dma((RING,)),
            dma((RING,)),
            dma((2,)),
            dma((3,)),
            dma(()),
            dma((4,)),
        ]
        return pl.pallas_call(
            functools.partial(gru_kernel, dims),
            name="gru",
            out_shape=(
                jax.ShapeDtypeStruct((steps, batch, part), BF16),
                jax.ShapeDtypeStruct((2, batch, part), F32),
            ),
            in_specs=specs,
            out_specs=(vmem, vmem),
            scratch_shapes=scratch,
            compiler_params=pltpu.CompilerParams(
                collective_id=0, has_side_effects=True, vmem_limit_bytes=61 * 1024 * 1024
            ),
        )(*operands)

    return jax.shard_map(
        device_body,
        mesh=mesh,
        in_specs=(seq_spec, seq_spec, wide_spec, wide_spec, square_spec, bias_spec, wide_spec, wide_spec, square_spec, bias_spec),
        out_specs=(out_spec, out_spec),
        check_vma=False,
    )
```

```python
import functools

import jax
import jax.numpy as jnp
from jax import lax
from jax.experimental import pallas as pl
from jax.experimental.pallas import tpu as pltpu
from jax.sharding import PartitionSpec as P

MESH = pl.DeviceIdType.MESH
F32 = jnp.float32
BF16 = jnp.bfloat16
LANES = 128

H1, H2, RH1, RH2 = 0, 2, 4, 5
R1, N1, R2, N2 = range(4)
XR, XU, XN, PR, PU, PN, U1, U2 = range(8)
RING = 4


def cdiv(a, b):
    return -(-a // b)


def hop(d, n):
    return min(d, n - d)


def nx_hops(nx, ny):
    return [hop(dx, nx) + hop(dy, ny) for dx in range(nx) for dy in range(ny) if (dx, dy) != (0, 0)]


def gru_kernel(dims, *refs):
    steps, batch, rows, cols, nx, ny, chunk = dims
    (x_hbm, h0, wx1, wru1, wn1, b1, wx2, wru2, wn2, b2,
     seq_out, fin_out,
     w_own, w_blk, w_upd, xb, hcat, h0s, state, ag_buf, hs, bias, bpad,
     p_u1, p_x, p_p, p_u2, s_u1, s_x, s_p, s_u2, xu_keep, pu_keep,
     raw, raw_n, tail, blk, out_n, out_s, fin_src, fin_buf, fblk, fin_n, fin_s,
     raw_sem, ld_sem, wl_sem, wsend, wrecv, pr_send, pr_recv, bs_send, bs_recv, x_sem, i_sem,
     ag_send, ag_recv, hs_send, hs_recv, rs_send, rs_recv, in_recv, f_sem, o_sem) = refs
    block = 2 * rows
    device_row = lax.axis_index("row")
    y = lax.axis_index("col")
    x = device_row // 2
    core = lax.rem(device_row, 2)

    def wrap(v, n):
        return lax.rem(v + n, n)

    def remote(src, dst, ssem, rsem, tx, tc, ty):
        return pltpu.make_async_remote_copy(
            src_ref=src, dst_ref=dst, send_sem=ssem, recv_sem=rsem,
            device_id={"row": tx * 2 + tc, "col": ty}, device_id_type=MESH,
        )

    def wait_in(dst, sem):
        pltpu.make_async_copy(dst, dst, sem).wait()

    offsets = [(dx, dy) for dx in range(nx) for dy in range(ny) if (dx, dy) != (0, 0)]
    offsets.sort(key=lambda o: hop(o[0], nx) + hop(o[1], ny))
    dists = [hop(dx, nx) + hop(dy, ny) for dx, dy in offsets]
    groups = []
    for d in sorted(set(dists)):
        first = dists.index(d)
        groups.append((first, first + dists.count(d)))
    peers = len(offsets)

    barrier = pltpu.get_barrier_semaphore()
    for d in range(1, 2 * nx * ny):
        tr = lax.rem(device_row + d % (2 * nx), 2 * nx)
        ty = lax.rem(y + d // (2 * nx), ny)
        pl.semaphore_signal(barrier, inc=1, device_id={"row": tr, "col": ty}, device_id_type=MESH)

    kept = ((wx1.at[0], XR), (wx1.at[2], XN), (wx1.at[1], XU), (None, U1),
            (wx2.at[0], PR), (wx2.at[2], PN), (wx2.at[1], PU), (None, U2))
    main = (block - (nx - 1) * chunk) // LANES * LANES

    def block_weight(u):
        return w_blk.at[u] if u < U1 else w_upd.at[u - U1]

    my_rows = pl.ds(pl.multiple_of(device_row * rows, 16), rows)

    def column_slice(i):
        return pl.ds(pl.multiple_of(i * chunk, LANES), chunk)

    size = raw.shape[1]
    jobs = [(l, n) for l in range(2) for n in range(rows // size)]

    def fetch(srcs, buf, sem, k):
        l, n = jobs[k]
        return pltpu.make_async_copy(srcs[l].at[pl.ds(n * size, size)], buf.at[k % 2], raw_sem.at[sem, k % 2])

    def fetch_first():
        for k in range(2):
            fetch((wru1, wru2), raw, 0, k).start()
            fetch((wn1, wn2), raw_n, 1, k).start()

    def split_gates(put):
        for k, (l, n) in enumerate(jobs):
            fetch((wru1, wru2), raw, 0, k).wait()

            def some(m, carry):
                both = jnp.transpose(raw[k % 2, pl.ds(pl.multiple_of(m * 16, 16), 16)], (1, 0, 2))
                put(l, n * size + m * 16, both[0], both[1])
                return carry
            lax.fori_loop(0, size // 16, some, 0)
            if k + 2 < len(jobs):
                fetch((wru1, wru2), raw, 0, k + 2).start()
            fetch((wn1, wn2), raw_n, 1, k).wait()
            rest = raw_n[k % 2, :, (nx - 1) * chunk + main:]
            tail[l, pl.ds(n * size, size)] = jnp.concatenate([rest, jnp.zeros((size, LANES - rest.shape[1]), BF16)], axis=1)
            if k + 2 < len(jobs):
                fetch((wn1, wn2), raw_n, 1, k + 2).start()

    def pieces(u, j, reset_source):
        l = 0 if u in (R1, N1) else 1
        if u in (R1, R2):
            return [(reset_source(l, j), pl.ds(0, chunk))]
        src = (wn1, wn2)[l]
        if j < nx - 1:
            return [(src.at[:, pl.ds(j * chunk, chunk)], pl.ds(0, chunk))]
        return [(src.at[:, pl.ds(j * chunk, main)], pl.ds(0, main)), (tail.at[l], pl.ds(main, LANES))]

    def move(u, reset_source, to_self):
        for tx in range(nx):
            for src, lanes in pieces(u, tx, reset_source):
                dst = w_own.at[u, my_rows, lanes]
                if to_self is None:
                    remote(src, dst, wsend.at[u], wrecv.at[u], tx, 1, y).start()
                else:
                    @pl.when(x != tx)
                    def _():
                        remote(src, dst, wsend.at[u], wrecv.at[u], tx, 1, y).start()

                    @pl.when(x == tx)
                    def _():
                        pltpu.make_async_copy(src, dst, to_self.at[u]).start()

    @pl.when(core == 0)
    def _():
        partner_rows = pl.ds(pl.multiple_of((device_row + 1) * rows, 16), rows)
        fetch_first()
        spare = lambda l, j: (nx * l + j) * rows
        w_upd[:, pl.ds(0, rows), pl.ds(nx * chunk - LANES, LANES)] = jnp.zeros((2, rows, LANES), BF16)
        for l in range(2):
            w_own[0, pl.ds(spare(l, nx - 1), rows), pl.ds(chunk - LANES, LANES)] = jnp.zeros((rows, LANES), BF16)

        def put(l, row, reset, update):
            w_upd[l, pl.ds(pl.multiple_of(row, 16), 16), 0:block] = update
            for j in range(nx):
                width = min(chunk, block - j * chunk)
                w_own[0, pl.ds(pl.multiple_of(spare(l, j) + row, 16), 16), 0:width] = reset[:, j * chunk:j * chunk + width]

        split_gates(put)
        reset_rows = lambda l, j: w_own.at[0, pl.ds(spare(l, j), rows)]
        xload = pltpu.make_async_copy(x_hbm, xb.at[0], x_sem.at[0])
        xload.start()
        for src, u in kept:
            if src is not None:
                pltpu.make_async_copy(src, block_weight(u).at[pl.ds(0, rows)], ld_sem.at[u]).start()
        pl.semaphore_wait(barrier, 2 * nx * ny - 1)

        @pl.when(x == y)
        def _():
            remote(h0, h0s, i_sem.at[0], i_sem.at[1], x, 1, y).start()

        move(R1, reset_rows, None)

        xload.wait()
        wait_in(xb.at[1], x_sem.at[1])

        def wait_kept(n):
            u = kept[n][1]
            if u < U1:
                wait_in(block_weight(u).at[pl.ds(0, rows)], ld_sem.at[u])
            wait_in(block_weight(u).at[pl.ds(rows, rows)], bs_recv.at[u])

        def row_dot(vec, u):
            return jnp.dot(vec, block_weight(u)[:, 0:block], preferred_element_type=F32)

        near_last = sorted(range(nx), key=lambda d: -hop(d, nx))

        def spread(src, dst, g, kind, slot):
            for d in near_last:
                tx = wrap(x + d, nx)
                remote(src.at[g, :, column_slice(tx)], dst.at[slot, x, g], rs_send.at[kind], in_recv.at[kind - 1, slot, g], tx, 1, y).start()

        def update_part(vec, u, kept_sum, kept_slot, src, dst, kind, slot):
            for d in near_last:
                tx = wrap(x + d, nx)
                src[0, :, column_slice(tx)] = (
                    jnp.dot(vec, block_weight(u)[:, column_slice(tx)], preferred_element_type=F32)
                    + kept_sum[kept_slot, :, column_slice(tx)])
                remote(src.at[:, :, column_slice(tx)], dst.at[slot, x], rs_send.at[kind], rs_recv.at[kind, slot], tx, 1, y).start()

        def spread_wait(src, kind):
            wait_in(src, rs_send.at[kind])

        def project(t):
            def half(g):
                return (jnp.dot(xb[0, t], w_blk[g, 0:rows], preferred_element_type=F32)
                        + jnp.dot(xb[1, t], w_blk[g, rows:block], preferred_element_type=F32))
            for g, u in enumerate((XR, XN)):
                s_x[g, :, 0:block] = half(u)
                spread(s_x, p_x, g, 1, lax.rem(t, RING))
            xu_keep[lax.rem(t, 2), :, 0:block] = half(XU)

        s_u1[...] = jnp.zeros_like(s_u1)
        s_u2[...] = jnp.zeros_like(s_u2)
        s_x[...] = jnp.zeros_like(s_x)
        s_p[...] = jnp.zeros_like(s_p)
        xu_keep[...] = jnp.zeros_like(xu_keep)
        pu_keep[...] = jnp.zeros_like(pu_keep)
        for n in range(3):
            wait_kept(n)
        project(0)
        move(N1, reset_rows, None)
        spread_wait(s_x, 1)
        project(1)
        for n in range(3, 8):
            wait_kept(n)

        def step(i, carry):
            @pl.when(i <= steps)
            def _():
                wait_in(hs.at[0, 0], hs_recv.at[0, lax.rem(i, RING)])

            @pl.when(i < steps)
            def _():
                @pl.when(i > 0)
                def _():
                    spread_wait(s_u1, 0)
                update_part(hs[0, lax.rem(i, RING), :, 0:block], U1, xu_keep, lax.rem(i, 2), s_u1, p_u1, 0, lax.rem(i, RING))

            @pl.when(jnp.logical_and(i >= 1, i <= steps))
            def _():
                h1v = hs[0, lax.rem(i, RING), :, 0:block]

                @pl.when(i > 1)
                def _():
                    spread_wait(s_p, 2)
                for g, u in enumerate((PR, PN)):
                    s_p[g, :, 0:block] = row_dot(h1v, u)
                    spread(s_p, p_p, g, 2, lax.rem(i + 3, RING))
                pu_keep[lax.rem(i + 1, 2), :, 0:block] = row_dot(h1v, PU)

            @pl.when(i >= 2)
            def _():
                wait_in(hs.at[1, 0], hs_recv.at[1, lax.rem(i, RING)])

                @pl.when(i > 2)
                def _():
                    spread_wait(s_u2, 3)
                update_part(hs[1, lax.rem(i, RING), :, 0:block], U2, pu_keep, lax.rem(i, 2), s_u2, p_u2, 3, lax.rem(i + 2, RING))

            @pl.when(i + 2 < steps)
            def _():
                spread_wait(s_x, 1)
                project(i + 2)

            for n, (u, at) in enumerate(((R2, 0), (N2, 1))):
                @pl.when(i == at)
                def _():
                    move(u, reset_rows, None)
                    wait_in(w_own.at[0, pl.ds(0, nx * rows)], pr_recv.at[n])
                    for tx in range(nx):
                        @pl.when(x != tx)
                        def _():
                            remote(w_own.at[1 + n, pl.ds(tx * rows, rows)], w_own.at[u, partner_rows],
                                   wsend.at[u], wrecv.at[u], tx, 1, y).start()
            return carry

        lax.fori_loop(0, steps + 2, step, 0)
        spread_wait(s_u1, 0)
        spread_wait(s_x, 1)
        spread_wait(s_p, 2)
        spread_wait(s_u2, 3)
        for u in range(4):
            wait_in(w_own.at[0, pl.ds(0, (nx if u in (R1, N1) else 2 * nx - 1) * rows)], wsend.at[u])

        @pl.when(x == y)
        def _():
            wait_in(h0, i_sem.at[0])
        wait_in(out_s, o_sem.at[1])
        wait_in(fin_s, o_sem.at[3])
        seq_out[...] = out_s[...]
        fin_out[...] = fin_s[...]

    @pl.when(core == 1)
    def _():
        fetch_first()
        w_upd[:, :, pl.ds(nx * chunk - LANES, LANES)] = jnp.zeros((2, 2 * rows, LANES), BF16)

        def put(l, row, reset, update):
            w_upd[l, pl.ds(pl.multiple_of(row, 16), 16), 0:block] = update
            w_upd[l, pl.ds(pl.multiple_of(rows + row, 16), 16), 0:block] = reset

        split_gates(put)
        reset_rows = lambda l, j: w_upd.at[l, pl.ds(rows, rows), pl.ds(j * chunk, chunk)]
        pl.semaphore_wait(barrier, 2 * nx * ny - 1)

        @pl.when(x == y)
        def _():
            wait_in(h0s, i_sem.at[1])
            hcat[...] = jnp.zeros_like(hcat)
            hcat[:, :, 0:rows] = h0s[...]
            hcat[:, :, rows:block] = h0[...]
            for d in range(1, nx):
                tx = wrap(x + d, nx)
                remote(hcat.at[:, :, column_slice(tx)], state, i_sem.at[2], i_sem.at[3], tx, 1, y).start()
            state[...] = hcat[:, :, column_slice(x)]
            wait_in(hcat.at[:, :, pl.ds(0, (nx - 1) * chunk)], i_sem.at[2])

        for u in (R1,):
            move(u, reset_rows, wl_sem)
        remote(x_hbm, xb.at[1], x_sem.at[0], x_sem.at[1], x, 0, y).start()
        for src, u in kept:
            if src is None:
                src = w_upd.at[u - U1, pl.ds(0, rows)]
            remote(src, block_weight(u).at[pl.ds(rows, rows)], bs_send.at[u], bs_recv.at[u], x, 0, y).start()
        for n, u in enumerate((R2, N2)):
            for tx in range(nx):
                for src, lanes in pieces(u, tx, reset_rows):
                    remote(src, w_own.at[1 + n, pl.ds(tx * rows, rows), lanes], pr_send.at[n], pr_recv.at[n], x, 0, y).start()

                    @pl.when(x == tx)
                    def _():
                        pltpu.make_async_copy(src, w_own.at[u, my_rows, lanes], wl_sem.at[u]).start()

        for u in range(4):
            w_own[u, pl.ds(nx * block, chunk * nx - block)] = jnp.zeros((chunk * nx - block, chunk), BF16)
        bpad[...] = jnp.zeros_like(bpad)
        bpad[0, 0:3, 0:block] = b1[...]
        bpad[1, 0:3, 0:block] = b2[...]
        bias[...] = bpad[:, :, column_slice(x)]
        valid = jnp.minimum(block - x * chunk, chunk)
        keep = lax.broadcasted_iota(jnp.int32, (batch, chunk), 1) < valid

        @pl.when(x != y)
        def _():
            wait_in(state, i_sem.at[3])

        def to_all(kind):
            for k in reversed(range(peers)):
                dx, dy = offsets[k]
                g = [j for j, (a, b) in enumerate(groups) if a <= k < b][0]
                remote(ag_buf.at[kind, 0, 0], ag_buf.at[kind, dy, dx], ag_send.at[kind], ag_recv.at[kind, g],
                       wrap(x + dx, nx), 1, wrap(y + dy, ny)).start()

        def to_block(layer, kind, slot):
            dy = wrap(y - x, ny)
            for dx in range(nx):
                remote(ag_buf.at[kind, dy, dx], hs.at[layer, slot, :, column_slice(wrap(x - dx, nx))],
                       hs_send.at[layer], hs_recv.at[layer, slot], x, 0, y).start()

        def chunks(n):
            return w_own.at[0, pl.ds(0, n * batch)]

        def sent(kind):
            wait_in(chunks(peers), ag_send.at[kind])

        def sent_blocks(layer):
            wait_in(chunks(nx), hs_send.at[layer])

        def weight_rows(dx, dy):
            sx, sy = wrap(x - dx, nx), wrap(y - dy, ny)
            return pl.ds(pl.multiple_of(sy * block + sx * chunk, 32), chunk)

        def arrive(kind, g):
            a, b = groups[g]
            wait_in(chunks(b - a), ag_recv.at[kind, g])

        def gathered_dot(kind, u, acc):
            acc = acc + jnp.dot(ag_buf[kind, 0, 0], w_own[u, weight_rows(0, 0)], preferred_element_type=F32)
            for g, (a, b) in enumerate(groups):
                arrive(kind, g)
                for dx, dy in offsets[a:b]:
                    acc = acc + jnp.dot(ag_buf[kind, dy, dx], w_own[u, weight_rows(dx, dy)], preferred_element_type=F32)
            return acc

        def partial_sum(buf, slot, g):
            total = buf[slot, 0, g]
            for s in range(1, nx):
                total = total + buf[slot, s, g]
            return total

        def wait_weights(u):
            wait_in(w_own.at[u, pl.ds(0, rows)], wl_sem.at[u])
            wait_in(w_own.at[u, pl.ds(0, (2 * nx - 1) * rows)], wrecv.at[u])

        for layer in range(2):
            kind = H1 if layer == 0 else H2
            ag_buf[kind, 0, 0] = jnp.where(keep, state[layer], 0.0).astype(BF16)
            to_all(kind)
        move(N1, reset_rows, wl_sem)

        def copy_row_block(kind):
            blk[:, column_slice(x)] = ag_buf[kind, 0, 0]
            for dx in range(1, nx):
                blk[:, column_slice(wrap(x - dx, nx))] = ag_buf[kind, 0, dx]

        def reset_phase(layer, kind, unit, slot, buf, sem, hslot):
            wait_in(buf.at[0, :, 0], sem.at[0])
            pre = gathered_dot(kind, unit, partial_sum(buf, slot, 0) + bias[layer, 0:1])
            to_block(layer, kind, hslot)
            if layer == 1:
                copy_row_block(kind)
            gate = jax.nn.sigmoid(pre)
            out = RH1 if layer == 0 else RH2
            ag_buf[out, 0, 0] = jnp.where(keep, gate * state[layer], 0.0).astype(BF16)
            to_all(out)
            sent(kind)

        def candidate_phase(layer, unit, slot, buf, ubuf, usem):
            kind = RH1 if layer == 0 else RH2
            wait_in(buf.at[0, :, 1], in_recv.at[layer, slot, 1])
            pre = gathered_dot(kind, unit, partial_sum(buf, slot, 1) + bias[layer, 2:3])
            cand = jnp.tanh(pre)
            wait_in(ubuf.at[0], usem)
            upd = jax.nn.sigmoid(partial_sum(ubuf, slot, 0) + bias[layer, 1:2])
            new = (1.0 - upd) * cand + upd * state[layer]
            state[layer] = new
            return jnp.where(keep, new, 0.0).astype(BF16)

        part = block // (2 * nx)

        def step(i, carry):
            slot1 = lax.rem(i, RING)
            t2 = i - 2
            slot2 = lax.rem(i + 2, RING)

            @pl.when(i < steps)
            def _():
                @pl.when(i == 0)
                def _():
                    wait_weights(R1)
                reset_phase(0, H1 + lax.rem(i, 2), R1, slot1, p_x, in_recv.at[0, slot1], slot1)

            @pl.when(i == steps)
            def _():
                kind = H1 + lax.rem(i, 2)
                for g in range(len(groups)):
                    arrive(kind, g)
                to_block(0, kind, slot1)
                sent(kind)

            @pl.when(t2 >= 0)
            def _():
                @pl.when(t2 == 0)
                def _():
                    wait_weights(R2)
                reset_phase(1, H2 + lax.rem(i, 2), R2, slot2, p_p, in_recv.at[1, slot2], slot1)

                @pl.when(t2 >= 1)
                def _():
                    for k in range(nx):
                        @pl.when(x == k)
                        def _():
                            out_s[t2 - 1] = blk[:, 2 * k * part:(2 * k + 1) * part]
                            out_n[t2 - 1] = blk[:, (2 * k + 1) * part:(2 * k + 2) * part]

            @pl.when(i < steps)
            def _():
                @pl.when(i == 0)
                def _():
                    wait_weights(N1)
                new = candidate_phase(0, N1, slot1, p_x, p_u1, rs_recv.at[0, slot1])
                ag_buf[H1 + lax.rem(i + 1, 2), 0, 0] = new
                to_all(H1 + lax.rem(i + 1, 2))
                sent(RH1)
                sent_blocks(0)

            @pl.when(t2 >= 0)
            def _():
                @pl.when(t2 == 0)
                def _():
                    wait_weights(N2)
                new = candidate_phase(1, N2, slot2, p_p, p_u2, rs_recv.at[3, slot2])

                @pl.when(t2 < steps - 1)
                def _():
                    ag_buf[H2 + lax.rem(i + 1, 2), 0, 0] = new
                    to_all(H2 + lax.rem(i + 1, 2))
                sent(RH2)
                sent_blocks(1)
            return carry

        lax.fori_loop(0, steps + 2, step, 0)
        sent_blocks(0)

        fin_src[...] = state[...]
        for d in range(1, nx):
            tx = wrap(x + d, nx)
            remote(fin_src, fin_buf.at[d], f_sem.at[0], f_sem.at[1], tx, 1, y).start()
        fblk[:, :, column_slice(x)] = state[...]
        wait_in(fin_buf.at[pl.ds(1, nx - 1)], f_sem.at[1])
        for d in range(1, nx):
            fblk[:, :, column_slice(wrap(x - d, nx))] = fin_buf[d]
        for k in range(nx):
            @pl.when(x == k)
            def _():
                s_part = fblk[:, :, 2 * k * part:(2 * k + 1) * part]
                n_part = fblk[:, :, (2 * k + 1) * part:(2 * k + 2) * part]
                fin_s[...] = s_part
                fin_n[...] = n_part
                out_s[steps - 1] = s_part[1].astype(BF16)
                out_n[steps - 1] = n_part[1].astype(BF16)
        remote(fin_s, fin_s, o_sem.at[2], o_sem.at[3], x, 0, y).start()
        remote(out_s, out_s, o_sem.at[0], o_sem.at[1], x, 0, y).start()
        seq_out[...] = out_n[...]
        fin_out[...] = fin_n[...]
        wait_in(fin_s, o_sem.at[2])
        wait_in(out_s, o_sem.at[0])
        wait_in(fin_buf.at[pl.ds(1, nx - 1)], f_sem.at[0])
        wait_in(xb.at[1], x_sem.at[0])
        for u in (R1, N1):
            wait_in(w_own.at[0, pl.ds(0, (nx - 1) * rows)], wsend.at[u])
        for n in range(2):
            wait_in(w_own.at[0, pl.ds(0, nx * rows)], pr_send.at[n])
        for u in range(8):
            wait_in(block_weight(u).at[pl.ds(rows, rows)], bs_send.at[u])


def solution(mesh):
    nx, ny = mesh.shape["row"] // 2, mesh.shape["col"]
    seq_spec = P(None, "data", "row")
    out_spec = P(None, "data", ("col", "row"))
    wide_spec = P("row", None, "col")
    square_spec = P("row", "col")
    bias_spec = P(None, "col")

    def device_body(x_rows, h_rows, wx_l1, whru_l1, whn_l1, bias_l1, wx_l2, whru_l2, whn_l2, bias_l2):
        steps, batch, rows = x_rows.shape
        cols = whn_l1.shape[1]
        chunk = cdiv(cdiv(cols, nx), LANES) * LANES
        wide = nx * chunk
        part = cols // (2 * nx)
        dims = (steps, batch, rows, cols, nx, ny, chunk)

        peers = nx * ny - 1
        total_rows = nx * cols
        hbm = pl.BlockSpec(memory_space=pl.ANY)
        vmem = pl.BlockSpec(memory_space=pltpu.VMEM)
        dma = pltpu.SemaphoreType.DMA
        operands = []
        specs = []
        for lead, wx, wru, wn, b in (((x_rows, h_rows), wx_l1, whru_l1, whn_l1, bias_l1), ((), wx_l2, whru_l2, whn_l2, bias_l2)):
            if lead:
                operands += list(lead)
                specs += [hbm, vmem]
            operands += [jnp.transpose(wx, (1, 0, 2)), wru, wn, b]
            specs += [hbm, hbm, hbm, vmem]
        scratch = [
            pltpu.VMEM((4, total_rows + wide - cols, chunk), BF16),
            pltpu.VMEM((6, 2 * rows, cols), BF16),
            pltpu.VMEM((2, 2 * rows, wide), BF16),
            pltpu.VMEM((2, steps, batch, rows), BF16),
            pltpu.VMEM((2, batch, wide), F32),
            pltpu.VMEM((2, batch, rows), F32),
            pltpu.VMEM((2, batch, chunk), F32),
            pltpu.VMEM((6, ny, nx, batch, chunk), BF16),
            pltpu.VMEM((2, RING, batch, wide), BF16),
            pltpu.VMEM((2, 8, chunk), F32),
            pltpu.VMEM((2, 8, wide), F32),
            pltpu.VMEM((RING, nx, 1, batch, chunk), F32),
            pltpu.VMEM((RING, nx, 2, batch, chunk), F32),
            pltpu.VMEM((RING, nx, 2, batch, chunk), F32),
            pltpu.VMEM((RING, nx, 1, batch, chunk), F32),
            pltpu.VMEM((1, batch, wide), F32),
            pltpu.VMEM((2, batch, wide), F32),
            pltpu.VMEM((2, batch, wide), F32),
            pltpu.VMEM((1, batch, wide), F32),
            pltpu.VMEM((2, batch, wide), F32),
            pltpu.VMEM((2, batch, wide), F32),
            pltpu.VMEM((2, rows // 3, 2, cols), BF16),
            pltpu.VMEM((2, rows // 3, cols), BF16),
            pltpu.VMEM((2, rows, LANES), BF16),
            pltpu.VMEM((batch, wide), BF16),
            pltpu.VMEM((steps, batch, part), BF16),
            pltpu.VMEM((steps, batch, part), BF16),
            pltpu.VMEM((2, batch, chunk), F32),
            pltpu.VMEM((nx, 2, batch, chunk), F32),
            pltpu.VMEM((2, batch, wide), F32),
            pltpu.VMEM((2, batch, part), F32),
            pltpu.VMEM((2, batch, part), F32),
            dma((2, 2)),
            dma((8,)),
            dma((4,)),
            dma((4,)),
            dma((4,)),
            dma((2,)),
            dma((2,)),
            dma((8,)),
            dma((8,)),
            dma((2,)),
            dma((4,)),
            dma((6,)),
            dma((6, len(set(nx_hops(nx, ny))))),
            dma((2,)),
            dma((2, RING)),
            dma((4,)),
            dma((4, RING)),
            dma((2, RING, 2)),
            dma((2,)),
            dma((4,)),
        ]
        return pl.pallas_call(
            functools.partial(gru_kernel, dims),
            name="gru",
            out_shape=(
                jax.ShapeDtypeStruct((steps, batch, part), BF16),
                jax.ShapeDtypeStruct((2, batch, part), F32),
            ),
            in_specs=specs,
            out_specs=(vmem, vmem),
            scratch_shapes=scratch,
            compiler_params=pltpu.CompilerParams(
                collective_id=0, has_side_effects=True, vmem_limit_bytes=67_000_000
            ),
        )(*operands)

    return jax.shard_map(
        device_body,
        mesh=mesh,
        in_specs=(seq_spec, seq_spec, wide_spec, wide_spec, square_spec, bias_spec, wide_spec, wide_spec, square_spec, bias_spec),
        out_specs=(out_spec, out_spec),
        check_vma=False,
    )
```

```python
import functools

import jax
import jax.numpy as jnp
from jax import lax
from jax.experimental import pallas as pl
from jax.experimental.pallas import tpu as pltpu
from jax.sharding import PartitionSpec as P

MESH = pl.DeviceIdType.MESH
F32 = jnp.float32
BF16 = jnp.bfloat16
LANES = 128

H1, H2, RH1, RH2 = 0, 2, 4, 5
R1, N1, R2, N2 = range(4)
XR, XU, XN, PR, PU, PN, U1, U2 = range(8)
RING = 4


def cdiv(a, b):
    return -(-a // b)


def hop(d, n):
    return min(d, n - d)


def nx_hops(nx, ny):
    return [hop(dx, nx) + hop(dy, ny) for dx in range(nx) for dy in range(ny) if (dx, dy) != (0, 0)]


def gru_kernel(dims, *refs):
    steps, batch, rows, cols, nx, ny, chunk = dims
    (x_hbm, h0, wx1, wru1, wn1, b1, wx2, wru2, wn2, b2,
     seq_out, fin_out,
     w_own, w_blk, w_upd, xb, hcat, h0s, state, ag_buf, hs, bias, bpad,
     p_u1, p_x, p_p, p_u2, s_u1, s_x, s_p, s_u2, xu_keep, pu_keep,
     raw, raw_n, tail, blk, out_n, out_s, fin_src, fin_buf, fblk, fin_n, fin_s,
     raw_sem, ld_sem, wl_sem, wsend, wrecv, pr_send, pr_recv, bs_send, bs_recv, x_sem, i_sem,
     ag_send, ag_recv, hs_send, hs_recv, rs_send, rs_recv, in_recv, f_sem, o_sem) = refs
    block = 2 * rows
    device_row = lax.axis_index("row")
    y = lax.axis_index("col")
    x = device_row // 2
    core = lax.rem(device_row, 2)

    def wrap(v, n):
        return lax.rem(v + n, n)

    def remote(src, dst, ssem, rsem, tx, tc, ty):
        return pltpu.make_async_remote_copy(
            src_ref=src, dst_ref=dst, send_sem=ssem, recv_sem=rsem,
            device_id={"row": tx * 2 + tc, "col": ty}, device_id_type=MESH,
        )

    def wait_in(dst, sem):
        pltpu.make_async_copy(dst, dst, sem).wait()

    offsets = [(dx, dy) for dx in range(nx) for dy in range(ny) if (dx, dy) != (0, 0)]
    offsets.sort(key=lambda o: hop(o[0], nx) + hop(o[1], ny))
    groups = ([(0, 4), (4, 10), (10, 15)], [(0, 4), (4, 15)])
    peers = len(offsets)

    barrier = pltpu.get_barrier_semaphore()
    for d in range(1, 2 * nx * ny):
        tr = lax.rem(device_row + d % (2 * nx), 2 * nx)
        ty = lax.rem(y + d // (2 * nx), ny)
        pl.semaphore_signal(barrier, inc=1, device_id={"row": tr, "col": ty}, device_id_type=MESH)

    kept = ((wx1.at[0], XR), (wx1.at[2], XN), (wx1.at[1], XU), (None, U1),
            (wx2.at[0], PR), (wx2.at[2], PN), (wx2.at[1], PU), (None, U2))
    main = (block - (nx - 1) * chunk) // LANES * LANES

    def block_weight(u):
        return w_blk.at[u] if u < U1 else w_upd.at[u - U1]

    my_rows = pl.ds(pl.multiple_of(device_row * rows, 16), rows)

    def column_slice(i):
        return pl.ds(pl.multiple_of(i * chunk, LANES), chunk)

    size = raw.shape[1]
    jobs = [(l, n) for l in range(2) for n in range(rows // size)]

    def fetch(srcs, buf, sem, k):
        l, n = jobs[k]
        return pltpu.make_async_copy(srcs[l].at[pl.ds(n * size, size)], buf.at[k % 2], raw_sem.at[sem, k % 2])

    def fetch_first():
        for k in range(2):
            fetch((wru1, wru2), raw, 0, k).start()
            fetch((wn1, wn2), raw_n, 1, k).start()

    def split_gates(put):
        for k, (l, n) in enumerate(jobs):
            fetch((wru1, wru2), raw, 0, k).wait()

            def some(m, carry):
                both = jnp.transpose(raw[k % 2, pl.ds(pl.multiple_of(m * 16, 16), 16)], (1, 0, 2))
                put(l, n * size + m * 16, both[0], both[1])
                return carry
            lax.fori_loop(0, size // 16, some, 0)
            if k + 2 < len(jobs):
                fetch((wru1, wru2), raw, 0, k + 2).start()
            fetch((wn1, wn2), raw_n, 1, k).wait()
            rest = raw_n[k % 2, :, (nx - 1) * chunk + main:]
            tail[l, pl.ds(n * size, size)] = jnp.concatenate([rest, jnp.zeros((size, LANES - rest.shape[1]), BF16)], axis=1)
            if k + 2 < len(jobs):
                fetch((wn1, wn2), raw_n, 1, k + 2).start()

    def pieces(u, j, reset_source):
        l = 0 if u in (R1, N1) else 1
        if u in (R1, R2):
            return [(reset_source(l, j), pl.ds(0, chunk))]
        src = (wn1, wn2)[l]
        if j < nx - 1:
            return [(src.at[:, pl.ds(j * chunk, chunk)], pl.ds(0, chunk))]
        return [(src.at[:, pl.ds(j * chunk, main)], pl.ds(0, main)), (tail.at[l], pl.ds(main, LANES))]

    def move(u, reset_source, to_self):
        for tx in range(nx):
            for src, lanes in pieces(u, tx, reset_source):
                dst = w_own.at[u, my_rows, lanes]
                if to_self is None:
                    remote(src, dst, wsend.at[u], wrecv.at[u], tx, 1, y).start()
                else:
                    @pl.when(x != tx)
                    def _():
                        remote(src, dst, wsend.at[u], wrecv.at[u], tx, 1, y).start()

                    @pl.when(x == tx)
                    def _():
                        pltpu.make_async_copy(src, dst, to_self.at[u]).start()

    @pl.when(core == 0)
    def _():
        partner_rows = pl.ds(pl.multiple_of((device_row + 1) * rows, 16), rows)
        fetch_first()
        spare = lambda l, j: (nx * l + j) * rows
        w_upd[:, pl.ds(0, rows), pl.ds(nx * chunk - LANES, LANES)] = jnp.zeros((2, rows, LANES), BF16)
        for l in range(2):
            w_own[0, pl.ds(spare(l, nx - 1), rows), pl.ds(chunk - LANES, LANES)] = jnp.zeros((rows, LANES), BF16)

        def put(l, row, reset, update):
            w_upd[l, pl.ds(pl.multiple_of(row, 16), 16), 0:block] = update
            for j in range(nx):
                width = min(chunk, block - j * chunk)
                w_own[0, pl.ds(pl.multiple_of(spare(l, j) + row, 16), 16), 0:width] = reset[:, j * chunk:j * chunk + width]

        split_gates(put)
        reset_rows = lambda l, j: w_own.at[0, pl.ds(spare(l, j), rows)]
        xload = pltpu.make_async_copy(x_hbm, xb.at[0], x_sem.at[0])
        xload.start()
        for src, u in kept:
            if src is not None:
                pltpu.make_async_copy(src, block_weight(u).at[pl.ds(0, rows)], ld_sem.at[u]).start()
        pl.semaphore_wait(barrier, 2 * nx * ny - 1)

        @pl.when(x == y)
        def _():
            remote(h0, h0s, i_sem.at[0], i_sem.at[1], x, 1, y).start()

        move(R1, reset_rows, None)

        xload.wait()
        wait_in(xb.at[1], x_sem.at[1])

        def wait_kept(n):
            u = kept[n][1]
            if u < U1:
                wait_in(block_weight(u).at[pl.ds(0, rows)], ld_sem.at[u])
            wait_in(block_weight(u).at[pl.ds(rows, rows)], bs_recv.at[u])

        def row_dot(vec, u):
            return jnp.dot(vec, block_weight(u)[:, 0:block], preferred_element_type=F32)

        near_last = sorted(range(nx), key=lambda d: -hop(d, nx))

        def spread(src, dst, g, kind, slot):
            for d in near_last:
                tx = wrap(x + d, nx)
                remote(src.at[g, :, column_slice(tx)], dst.at[slot, x, g], rs_send.at[kind], in_recv.at[kind - 1, slot, g], tx, 1, y).start()

        def update_part(vec, u, kept_sum, kept_slot, src, dst, kind, slot):
            for d in near_last:
                tx = wrap(x + d, nx)
                src[0, :, column_slice(tx)] = (
                    jnp.dot(vec, block_weight(u)[:, column_slice(tx)], preferred_element_type=F32)
                    + kept_sum[kept_slot, :, column_slice(tx)])
                remote(src.at[:, :, column_slice(tx)], dst.at[slot, x], rs_send.at[kind], rs_recv.at[kind, slot], tx, 1, y).start()

        def spread_wait(src, kind):
            wait_in(src, rs_send.at[kind])

        def project(t):
            def half(g):
                return (jnp.dot(xb[0, t], w_blk[g, 0:rows], preferred_element_type=F32)
                        + jnp.dot(xb[1, t], w_blk[g, rows:block], preferred_element_type=F32))
            for g, u in enumerate((XR, XN)):
                s_x[g, :, 0:block] = half(u)
                spread(s_x, p_x, g, 1, lax.rem(t, RING))
            xu_keep[lax.rem(t, 2), :, 0:block] = half(XU)

        s_u1[...] = jnp.zeros_like(s_u1)
        s_u2[...] = jnp.zeros_like(s_u2)
        s_x[...] = jnp.zeros_like(s_x)
        s_p[...] = jnp.zeros_like(s_p)
        xu_keep[...] = jnp.zeros_like(xu_keep)
        pu_keep[...] = jnp.zeros_like(pu_keep)
        for n in range(3):
            wait_kept(n)
        project(0)
        move(N1, reset_rows, None)
        spread_wait(s_x, 1)
        project(1)
        for n in range(3, 8):
            wait_kept(n)

        def step(i, carry):
            @pl.when(i <= steps)
            def _():
                wait_in(hs.at[0, 0], hs_recv.at[0, lax.rem(i, RING)])

            @pl.when(i < steps)
            def _():
                @pl.when(i > 0)
                def _():
                    spread_wait(s_u1, 0)
                update_part(hs[0, lax.rem(i, RING), :, 0:block], U1, xu_keep, lax.rem(i, 2), s_u1, p_u1, 0, lax.rem(i, RING))

            @pl.when(jnp.logical_and(i >= 1, i <= steps))
            def _():
                h1v = hs[0, lax.rem(i, RING), :, 0:block]

                @pl.when(i > 1)
                def _():
                    spread_wait(s_p, 2)
                s_p[0, :, 0:block] = row_dot(h1v, PR)
                spread(s_p, p_p, 0, 2, lax.rem(i + 3, RING))

            @pl.when(i >= 2)
            def _():
                wait_in(hs.at[1, 0], hs_recv.at[1, lax.rem(i, RING)])

                @pl.when(i > 2)
                def _():
                    spread_wait(s_u2, 3)
                update_part(hs[1, lax.rem(i, RING), :, 0:block], U2, pu_keep, lax.rem(i, 2), s_u2, p_u2, 3, lax.rem(i + 2, RING))

            @pl.when(jnp.logical_and(i >= 1, i <= steps))
            def _():
                s_p[1, :, 0:block] = row_dot(hs[0, lax.rem(i, RING), :, 0:block], PN)
                spread(s_p, p_p, 1, 2, lax.rem(i + 3, RING))

            @pl.when(jnp.logical_and(i >= 1, i <= steps))
            def _():
                pu_keep[lax.rem(i + 1, 2), :, 0:block] = row_dot(hs[0, lax.rem(i, RING), :, 0:block], PU)

            @pl.when(i + 2 < steps)
            def _():
                spread_wait(s_x, 1)
                project(i + 2)

            for n, (u, at) in enumerate(((R2, 0), (N2, 1))):
                @pl.when(i == at)
                def _():
                    move(u, reset_rows, None)
                    wait_in(w_own.at[0, pl.ds(0, nx * rows)], pr_recv.at[n])
                    for tx in range(nx):
                        @pl.when(x != tx)
                        def _():
                            remote(w_own.at[1 + n, pl.ds(tx * rows, rows)], w_own.at[u, partner_rows],
                                   wsend.at[u], wrecv.at[u], tx, 1, y).start()
            return carry

        lax.fori_loop(0, steps + 2, step, 0)
        spread_wait(s_u1, 0)
        spread_wait(s_x, 1)
        spread_wait(s_p, 2)
        spread_wait(s_u2, 3)
        for u in range(4):
            wait_in(w_own.at[0, pl.ds(0, (nx if u in (R1, N1) else 2 * nx - 1) * rows)], wsend.at[u])

        @pl.when(x == y)
        def _():
            wait_in(h0, i_sem.at[0])
        wait_in(out_s, o_sem.at[1])
        wait_in(fin_s, o_sem.at[3])
        seq_out[...] = out_s[...]
        fin_out[...] = fin_s[...]

    @pl.when(core == 1)
    def _():
        fetch_first()
        w_upd[:, :, pl.ds(nx * chunk - LANES, LANES)] = jnp.zeros((2, 2 * rows, LANES), BF16)

        def put(l, row, reset, update):
            w_upd[l, pl.ds(pl.multiple_of(row, 16), 16), 0:block] = update
            w_upd[l, pl.ds(pl.multiple_of(rows + row, 16), 16), 0:block] = reset

        split_gates(put)
        reset_rows = lambda l, j: w_upd.at[l, pl.ds(rows, rows), pl.ds(j * chunk, chunk)]
        pl.semaphore_wait(barrier, 2 * nx * ny - 1)

        @pl.when(x == y)
        def _():
            wait_in(h0s, i_sem.at[1])
            hcat[...] = jnp.zeros_like(hcat)
            hcat[:, :, 0:rows] = h0s[...]
            hcat[:, :, rows:block] = h0[...]
            for d in range(1, nx):
                tx = wrap(x + d, nx)
                remote(hcat.at[:, :, column_slice(tx)], state, i_sem.at[2], i_sem.at[3], tx, 1, y).start()
            state[...] = hcat[:, :, column_slice(x)]
            wait_in(hcat.at[:, :, pl.ds(0, (nx - 1) * chunk)], i_sem.at[2])

        for u in (R1,):
            move(u, reset_rows, wl_sem)
        remote(x_hbm, xb.at[1], x_sem.at[0], x_sem.at[1], x, 0, y).start()
        for src, u in kept:
            if src is None:
                src = w_upd.at[u - U1, pl.ds(0, rows)]
            remote(src, block_weight(u).at[pl.ds(rows, rows)], bs_send.at[u], bs_recv.at[u], x, 0, y).start()
        for n, u in enumerate((R2, N2)):
            for tx in range(nx):
                for src, lanes in pieces(u, tx, reset_rows):
                    remote(src, w_own.at[1 + n, pl.ds(tx * rows, rows), lanes], pr_send.at[n], pr_recv.at[n], x, 0, y).start()

                    @pl.when(x == tx)
                    def _():
                        pltpu.make_async_copy(src, w_own.at[u, my_rows, lanes], wl_sem.at[u]).start()

        for u in range(4):
            w_own[u, pl.ds(nx * block, chunk * nx - block)] = jnp.zeros((chunk * nx - block, chunk), BF16)
        bpad[...] = jnp.zeros_like(bpad)
        bpad[0, 0:3, 0:block] = b1[...]
        bpad[1, 0:3, 0:block] = b2[...]
        bias[...] = bpad[:, :, column_slice(x)]
        valid = jnp.minimum(block - x * chunk, chunk)
        keep = lax.broadcasted_iota(jnp.int32, (batch, chunk), 1) < valid

        @pl.when(x != y)
        def _():
            wait_in(state, i_sem.at[3])

        def to_all(layer, kind):
            for k in reversed(range(peers)):
                dx, dy = offsets[k]
                g = [j for j, (a, b) in enumerate(groups[layer]) if a <= k < b][0]
                remote(ag_buf.at[kind, 0, 0], ag_buf.at[kind, dy, dx], ag_send.at[kind], ag_recv.at[kind, g],
                       wrap(x + dx, nx), 1, wrap(y + dy, ny)).start()

        def to_block(layer, kind, slot):
            dy = wrap(y - x, ny)
            for dx in range(nx):
                remote(ag_buf.at[kind, dy, dx], hs.at[layer, slot, :, column_slice(wrap(x - dx, nx))],
                       hs_send.at[layer], hs_recv.at[layer, slot], x, 0, y).start()

        def chunks(n):
            return w_own.at[0, pl.ds(0, n * batch)]

        def sent(kind):
            wait_in(chunks(peers), ag_send.at[kind])

        def sent_blocks(layer):
            wait_in(chunks(nx), hs_send.at[layer])

        def weight_rows(dx, dy):
            sx, sy = wrap(x - dx, nx), wrap(y - dy, ny)
            return pl.ds(pl.multiple_of(sy * block + sx * chunk, 32), chunk)

        def arrive(layer, kind, g):
            a, b = groups[layer][g]
            wait_in(chunks(b - a), ag_recv.at[kind, g])

        def gathered_dot(layer, kind, u, acc, then=None):
            acc = acc + jnp.dot(ag_buf[kind, 0, 0], w_own[u, weight_rows(0, 0)], preferred_element_type=F32)
            for g, (a, b) in enumerate(groups[layer]):
                arrive(layer, kind, g)
                if g == len(groups[layer]) - 1 and then is not None:
                    then()
                for dx, dy in offsets[a:b]:
                    acc = acc + jnp.dot(ag_buf[kind, dy, dx], w_own[u, weight_rows(dx, dy)], preferred_element_type=F32)
            return acc

        def partial_sum(buf, slot, g):
            total = buf[slot, 0, g]
            for s in range(1, nx):
                total = total + buf[slot, s, g]
            return total

        def wait_weights(u):
            wait_in(w_own.at[u, pl.ds(0, rows)], wl_sem.at[u])
            wait_in(w_own.at[u, pl.ds(0, (2 * nx - 1) * rows)], wrecv.at[u])

        for layer in range(2):
            kind = H1 if layer == 0 else H2
            ag_buf[kind, 0, 0] = jnp.where(keep, state[layer], 0.0).astype(BF16)
            to_all(layer, kind)
        move(N1, reset_rows, wl_sem)

        def copy_row_block(kind):
            blk[:, column_slice(x)] = ag_buf[kind, 0, 0]
            for dx in range(1, nx):
                blk[:, column_slice(wrap(x - dx, nx))] = ag_buf[kind, 0, dx]

        def reset_phase(layer, kind, unit, slot, buf, sem, hslot):
            wait_in(buf.at[0, :, 0], sem.at[0])
            pre = gathered_dot(layer, kind, unit, partial_sum(buf, slot, 0) + bias[layer, 0:1],
                               functools.partial(to_block, layer, kind, hslot))
            if layer == 1:
                copy_row_block(kind)
            gate = jax.nn.sigmoid(pre)
            out = RH1 if layer == 0 else RH2
            ag_buf[out, 0, 0] = jnp.where(keep, gate * state[layer], 0.0).astype(BF16)
            to_all(layer, out)
            sent(kind)

        def candidate_phase(layer, unit, slot, buf, ubuf, usem):
            kind = RH1 if layer == 0 else RH2
            wait_in(buf.at[0, :, 1], in_recv.at[layer, slot, 1])
            pre = gathered_dot(layer, kind, unit, partial_sum(buf, slot, 1) + bias[layer, 2:3])
            cand = jnp.tanh(pre)
            wait_in(ubuf.at[0], usem)
            upd = jax.nn.sigmoid(partial_sum(ubuf, slot, 0) + bias[layer, 1:2])
            new = (1.0 - upd) * cand + upd * state[layer]
            state[layer] = new
            return jnp.where(keep, new, 0.0).astype(BF16)

        part = block // (2 * nx)

        def step(i, carry):
            slot1 = lax.rem(i, RING)
            t2 = i - 2
            slot2 = lax.rem(i + 2, RING)

            @pl.when(i < steps)
            def _():
                @pl.when(i == 0)
                def _():
                    wait_weights(R1)
                reset_phase(0, H1 + lax.rem(i, 2), R1, slot1, p_x, in_recv.at[0, slot1], slot1)

            @pl.when(i == steps)
            def _():
                kind = H1 + lax.rem(i, 2)
                for g in range(len(groups[0])):
                    arrive(0, kind, g)
                to_block(0, kind, slot1)
                sent(kind)

            @pl.when(t2 >= 0)
            def _():
                @pl.when(t2 == 0)
                def _():
                    wait_weights(R2)
                reset_phase(1, H2 + lax.rem(i, 2), R2, slot2, p_p, in_recv.at[1, slot2], slot1)

                @pl.when(t2 >= 1)
                def _():
                    for k in range(nx):
                        @pl.when(x == k)
                        def _():
                            out_s[t2 - 1] = blk[:, 2 * k * part:(2 * k + 1) * part]
                            out_n[t2 - 1] = blk[:, (2 * k + 1) * part:(2 * k + 2) * part]

            @pl.when(i < steps)
            def _():
                @pl.when(i == 0)
                def _():
                    wait_weights(N1)
                new = candidate_phase(0, N1, slot1, p_x, p_u1, rs_recv.at[0, slot1])
                ag_buf[H1 + lax.rem(i + 1, 2), 0, 0] = new
                to_all(0, H1 + lax.rem(i + 1, 2))
                sent(RH1)
                sent_blocks(0)

            @pl.when(t2 >= 0)
            def _():
                @pl.when(t2 == 0)
                def _():
                    wait_weights(N2)
                new = candidate_phase(1, N2, slot2, p_p, p_u2, rs_recv.at[3, slot2])

                @pl.when(t2 < steps - 1)
                def _():
                    ag_buf[H2 + lax.rem(i + 1, 2), 0, 0] = new
                    to_all(1, H2 + lax.rem(i + 1, 2))
                sent(RH2)
                sent_blocks(1)
            return carry

        lax.fori_loop(0, steps + 2, step, 0)
        sent_blocks(0)

        fin_src[...] = state[...]
        for d in range(1, nx):
            tx = wrap(x + d, nx)
            remote(fin_src, fin_buf.at[d], f_sem.at[0], f_sem.at[1], tx, 1, y).start()
        fblk[:, :, column_slice(x)] = state[...]
        wait_in(fin_buf.at[pl.ds(1, nx - 1)], f_sem.at[1])
        for d in range(1, nx):
            fblk[:, :, column_slice(wrap(x - d, nx))] = fin_buf[d]
        for k in range(nx):
            @pl.when(x == k)
            def _():
                s_part = fblk[:, :, 2 * k * part:(2 * k + 1) * part]
                n_part = fblk[:, :, (2 * k + 1) * part:(2 * k + 2) * part]
                fin_s[...] = s_part
                fin_n[...] = n_part
                out_s[steps - 1] = s_part[1].astype(BF16)
                out_n[steps - 1] = n_part[1].astype(BF16)
        remote(fin_s, fin_s, o_sem.at[2], o_sem.at[3], x, 0, y).start()
        remote(out_s, out_s, o_sem.at[0], o_sem.at[1], x, 0, y).start()
        seq_out[...] = out_n[...]
        fin_out[...] = fin_n[...]
        wait_in(fin_s, o_sem.at[2])
        wait_in(out_s, o_sem.at[0])
        wait_in(fin_buf.at[pl.ds(1, nx - 1)], f_sem.at[0])
        wait_in(xb.at[1], x_sem.at[0])
        for u in (R1, N1):
            wait_in(w_own.at[0, pl.ds(0, (nx - 1) * rows)], wsend.at[u])
        for n in range(2):
            wait_in(w_own.at[0, pl.ds(0, nx * rows)], pr_send.at[n])
        for u in range(8):
            wait_in(block_weight(u).at[pl.ds(rows, rows)], bs_send.at[u])


def solution(mesh):
    nx, ny = mesh.shape["row"] // 2, mesh.shape["col"]
    seq_spec = P(None, "data", "row")
    out_spec = P(None, "data", ("col", "row"))
    wide_spec = P("row", None, "col")
    square_spec = P("row", "col")
    bias_spec = P(None, "col")

    def device_body(x_rows, h_rows, wx_l1, whru_l1, whn_l1, bias_l1, wx_l2, whru_l2, whn_l2, bias_l2):
        steps, batch, rows = x_rows.shape
        cols = whn_l1.shape[1]
        chunk = cdiv(cdiv(cols, nx), LANES) * LANES
        wide = nx * chunk
        part = cols // (2 * nx)
        dims = (steps, batch, rows, cols, nx, ny, chunk)

        peers = nx * ny - 1
        total_rows = nx * cols
        hbm = pl.BlockSpec(memory_space=pl.ANY)
        vmem = pl.BlockSpec(memory_space=pltpu.VMEM)
        dma = pltpu.SemaphoreType.DMA
        operands = []
        specs = []
        for lead, wx, wru, wn, b in (((x_rows, h_rows), wx_l1, whru_l1, whn_l1, bias_l1), ((), wx_l2, whru_l2, whn_l2, bias_l2)):
            if lead:
                operands += list(lead)
                specs += [hbm, vmem]
            operands += [jnp.transpose(wx, (1, 0, 2)), wru, wn, b]
            specs += [hbm, hbm, hbm, vmem]
        scratch = [
            pltpu.VMEM((4, total_rows + wide - cols, chunk), BF16),
            pltpu.VMEM((6, 2 * rows, cols), BF16),
            pltpu.VMEM((2, 2 * rows, wide), BF16),
            pltpu.VMEM((2, steps, batch, rows), BF16),
            pltpu.VMEM((2, batch, wide), F32),
            pltpu.VMEM((2, batch, rows), F32),
            pltpu.VMEM((2, batch, chunk), F32),
            pltpu.VMEM((6, ny, nx, batch, chunk), BF16),
            pltpu.VMEM((2, RING, batch, wide), BF16),
            pltpu.VMEM((2, 8, chunk), F32),
            pltpu.VMEM((2, 8, wide), F32),
            pltpu.VMEM((RING, nx, 1, batch, chunk), F32),
            pltpu.VMEM((RING, nx, 2, batch, chunk), F32),
            pltpu.VMEM((RING, nx, 2, batch, chunk), F32),
            pltpu.VMEM((RING, nx, 1, batch, chunk), F32),
            pltpu.VMEM((1, batch, wide), F32),
            pltpu.VMEM((2, batch, wide), F32),
            pltpu.VMEM((2, batch, wide), F32),
            pltpu.VMEM((1, batch, wide), F32),
            pltpu.VMEM((2, batch, wide), F32),
            pltpu.VMEM((2, batch, wide), F32),
            pltpu.VMEM((2, rows // 3, 2, cols), BF16),
            pltpu.VMEM((2, rows // 3, cols), BF16),
            pltpu.VMEM((2, rows, LANES), BF16),
            pltpu.VMEM((batch, wide), BF16),
            pltpu.VMEM((steps, batch, part), BF16),
            pltpu.VMEM((steps, batch, part), BF16),
            pltpu.VMEM((2, batch, chunk), F32),
            pltpu.VMEM((nx, 2, batch, chunk), F32),
            pltpu.VMEM((2, batch, wide), F32),
            pltpu.VMEM((2, batch, part), F32),
            pltpu.VMEM((2, batch, part), F32),
            dma((2, 2)),
            dma((8,)),
            dma((4,)),
            dma((4,)),
            dma((4,)),
            dma((2,)),
            dma((2,)),
            dma((8,)),
            dma((8,)),
            dma((2,)),
            dma((4,)),
            dma((6,)),
            dma((6, 4)),
            dma((2,)),
            dma((2, RING)),
            dma((4,)),
            dma((4, RING)),
            dma((2, RING, 2)),
            dma((2,)),
            dma((4,)),
        ]
        return pl.pallas_call(
            functools.partial(gru_kernel, dims),
            name="gru",
            out_shape=(
                jax.ShapeDtypeStruct((steps, batch, part), BF16),
                jax.ShapeDtypeStruct((2, batch, part), F32),
            ),
            in_specs=specs,
            out_specs=(vmem, vmem),
            scratch_shapes=scratch,
            compiler_params=pltpu.CompilerParams(
                collective_id=0, has_side_effects=True, vmem_limit_bytes=67_000_000
            ),
        )(*operands)

    return jax.shard_map(
        device_body,
        mesh=mesh,
        in_specs=(seq_spec, seq_spec, wide_spec, wide_spec, square_spec, bias_spec, wide_spec, wide_spec, square_spec, bias_spec),
        out_specs=(out_spec, out_spec),
        check_vma=False,
    )
```

```python
import functools

import jax
import jax.numpy as jnp
from jax import lax
from jax.experimental import pallas as pl
from jax.experimental.pallas import tpu as pltpu
from jax.sharding import PartitionSpec as P

MESH = pl.DeviceIdType.MESH
F32 = jnp.float32
BF16 = jnp.bfloat16
LANES = 128

H1, H2, RH1, RH2 = 0, 2, 4, 5
R1, N1, R2, N2 = range(4)
XR, XU, XN, PR, PU, PN, U1, U2 = range(8)
RING = 4


def cdiv(a, b):
    return -(-a // b)


def hop(d, n):
    return min(d, n - d)


def nx_hops(nx, ny):
    return [hop(dx, nx) + hop(dy, ny) for dx in range(nx) for dy in range(ny) if (dx, dy) != (0, 0)]


def gru_kernel(dims, *refs):
    steps, batch, rows, cols, nx, ny, chunk = dims
    (x_hbm, h0, wx1, wru1, wn1, b1, wx2, wru2, wn2, b2,
     seq_out, fin_out,
     w_own, w_blk, w_upd, xb, hcat, h0s, state, ag_buf, hs, bias, bpad,
     p_u1, p_x, p_p, p_u2, s_u1, s_x, s_p, s_u2, xu_keep, pu_keep,
     raw, raw_n, tail, blk, out_n, out_s, fin_src, fin_buf, fblk, fin_n, fin_s,
     raw_sem, ld_sem, wl_sem, wsend, wrecv, pr_send, pr_recv, bs_send, bs_recv, x_sem, i_sem,
     ag_send, ag_recv, hs_send, hs_recv, rs_send, rs_recv, in_recv, f_sem, o_sem) = refs
    block = 2 * rows
    device_row = lax.axis_index("row")
    y = lax.axis_index("col")
    x = device_row // 2
    core = lax.rem(device_row, 2)

    def wrap(v, n):
        return lax.rem(v + n, n)

    def remote(src, dst, ssem, rsem, tx, tc, ty):
        return pltpu.make_async_remote_copy(
            src_ref=src, dst_ref=dst, send_sem=ssem, recv_sem=rsem,
            device_id={"row": tx * 2 + tc, "col": ty}, device_id_type=MESH,
        )

    def wait_in(dst, sem):
        pltpu.make_async_copy(dst, dst, sem).wait()

    offsets = [(dx, dy) for dx in range(nx) for dy in range(ny) if (dx, dy) != (0, 0)]
    offsets.sort(key=lambda o: hop(o[0], nx) + hop(o[1], ny))
    groups = ([(0, 4), (4, 10), (10, 15)], [(0, 5), (5, 15)])
    peers = len(offsets)
    send_order = sorted(
        (o for o in offsets if o[0] and o[1]), key=lambda o: (-hop(o[0], nx) - hop(o[1], ny), -hop(o[1], ny), o[1], o[0]))
    send_order += sorted((o for o in offsets if not o[1]), key=lambda o: (hop(o[0], nx), o[0]))
    send_order += sorted((o for o in offsets if not o[0]), key=lambda o: (-hop(o[1], ny), o[1]))

    barrier = pltpu.get_barrier_semaphore()
    for d in range(1, 2 * nx * ny):
        tr = lax.rem(device_row + d % (2 * nx), 2 * nx)
        ty = lax.rem(y + d // (2 * nx), ny)
        pl.semaphore_signal(barrier, inc=1, device_id={"row": tr, "col": ty}, device_id_type=MESH)

    kept = ((wx1.at[0], XR), (wx1.at[2], XN), (wx1.at[1], XU), (None, U1),
            (wx2.at[0], PR), (wx2.at[2], PN), (wx2.at[1], PU), (None, U2))
    main = (block - (nx - 1) * chunk) // LANES * LANES

    def block_weight(u):
        return w_blk.at[u] if u < U1 else w_upd.at[u - U1]

    my_rows = pl.ds(pl.multiple_of(device_row * rows, 16), rows)

    def column_slice(i):
        return pl.ds(pl.multiple_of(i * chunk, LANES), chunk)

    size = raw.shape[1]
    jobs = [(l, n) for l in range(2) for n in range(rows // size)]

    def fetch(srcs, buf, sem, k):
        l, n = jobs[k]
        return pltpu.make_async_copy(srcs[l].at[pl.ds(n * size, size)], buf.at[k % 2], raw_sem.at[sem, k % 2])

    def fetch_first():
        for k in range(2):
            fetch((wru1, wru2), raw, 0, k).start()
            fetch((wn1, wn2), raw_n, 1, k).start()

    def split_gates(put):
        for k, (l, n) in enumerate(jobs):
            fetch((wru1, wru2), raw, 0, k).wait()

            def some(m, carry):
                both = jnp.transpose(raw[k % 2, pl.ds(pl.multiple_of(m * 16, 16), 16)], (1, 0, 2))
                put(l, n * size + m * 16, both[0], both[1])
                return carry
            lax.fori_loop(0, size // 16, some, 0)
            if k + 2 < len(jobs):
                fetch((wru1, wru2), raw, 0, k + 2).start()
            fetch((wn1, wn2), raw_n, 1, k).wait()
            rest = raw_n[k % 2, :, (nx - 1) * chunk + main:]
            tail[l, pl.ds(n * size, size)] = jnp.concatenate([rest, jnp.zeros((size, LANES - rest.shape[1]), BF16)], axis=1)
            if k + 2 < len(jobs):
                fetch((wn1, wn2), raw_n, 1, k + 2).start()

    def pieces(u, j, reset_source):
        l = 0 if u in (R1, N1) else 1
        if u in (R1, R2):
            return [(reset_source(l, j), pl.ds(0, chunk))]
        src = (wn1, wn2)[l]
        if j < nx - 1:
            return [(src.at[:, pl.ds(j * chunk, chunk)], pl.ds(0, chunk))]
        return [(src.at[:, pl.ds(j * chunk, main)], pl.ds(0, main)), (tail.at[l], pl.ds(main, LANES))]

    def move(u, reset_source, to_self):
        for tx in range(nx):
            for src, lanes in pieces(u, tx, reset_source):
                dst = w_own.at[u, my_rows, lanes]
                if to_self is None:
                    remote(src, dst, wsend.at[u], wrecv.at[u], tx, 1, y).start()
                else:
                    @pl.when(x != tx)
                    def _():
                        remote(src, dst, wsend.at[u], wrecv.at[u], tx, 1, y).start()

                    @pl.when(x == tx)
                    def _():
                        pltpu.make_async_copy(src, dst, to_self.at[u]).start()

    @pl.when(core == 0)
    def _():
        partner_rows = pl.ds(pl.multiple_of((device_row + 1) * rows, 16), rows)
        fetch_first()
        spare = lambda l, j: (nx * l + j) * rows
        w_upd[:, pl.ds(0, rows), pl.ds(nx * chunk - LANES, LANES)] = jnp.zeros((2, rows, LANES), BF16)
        for l in range(2):
            w_own[0, pl.ds(spare(l, nx - 1), rows), pl.ds(chunk - LANES, LANES)] = jnp.zeros((rows, LANES), BF16)

        def put(l, row, reset, update):
            w_upd[l, pl.ds(pl.multiple_of(row, 16), 16), 0:block] = update
            for j in range(nx):
                width = min(chunk, block - j * chunk)
                w_own[0, pl.ds(pl.multiple_of(spare(l, j) + row, 16), 16), 0:width] = reset[:, j * chunk:j * chunk + width]

        split_gates(put)
        reset_rows = lambda l, j: w_own.at[0, pl.ds(spare(l, j), rows)]
        xload = pltpu.make_async_copy(x_hbm, xb.at[0], x_sem.at[0])
        xload.start()
        for src, u in kept:
            if src is not None:
                pltpu.make_async_copy(src, block_weight(u).at[pl.ds(0, rows)], ld_sem.at[u]).start()
        pl.semaphore_wait(barrier, 2 * nx * ny - 1)

        @pl.when(x == y)
        def _():
            remote(h0, h0s, i_sem.at[0], i_sem.at[1], x, 1, y).start()

        move(R1, reset_rows, None)

        xload.wait()
        wait_in(xb.at[1], x_sem.at[1])

        def wait_kept(n):
            u = kept[n][1]
            if u < U1:
                wait_in(block_weight(u).at[pl.ds(0, rows)], ld_sem.at[u])
            wait_in(block_weight(u).at[pl.ds(rows, rows)], bs_recv.at[u])

        def row_dot(vec, u):
            return jnp.dot(vec, block_weight(u)[:, 0:block], preferred_element_type=F32)

        near_last = sorted(range(nx), key=lambda d: (-hop(d, nx), -d))

        def spread(src, dst, g, kind, slot):
            for d in near_last:
                tx = wrap(x + d, nx)
                remote(src.at[g, :, column_slice(tx)], dst.at[slot, x, g], rs_send.at[kind], in_recv.at[kind - 1, slot, g], tx, 1, y).start()

        def update_part(vec, u, kept_sum, kept_slot, src, dst, kind, slot):
            for d in near_last:
                tx = wrap(x + d, nx)
                src[0, :, column_slice(tx)] = (
                    jnp.dot(vec, block_weight(u)[:, column_slice(tx)], preferred_element_type=F32)
                    + kept_sum[kept_slot, :, column_slice(tx)])
                remote(src.at[:, :, column_slice(tx)], dst.at[slot, x], rs_send.at[kind], rs_recv.at[kind, slot], tx, 1, y).start()

        def spread_wait(src, kind):
            wait_in(src, rs_send.at[kind])

        def project(t):
            def half(g):
                return (jnp.dot(xb[0, t], w_blk[g, 0:rows], preferred_element_type=F32)
                        + jnp.dot(xb[1, t], w_blk[g, rows:block], preferred_element_type=F32))
            for g, u in enumerate((XR, XN)):
                s_x[g, :, 0:block] = half(u)
                spread(s_x, p_x, g, 1, lax.rem(t, RING))
            xu_keep[lax.rem(t, 2), :, 0:block] = half(XU)

        s_u1[...] = jnp.zeros_like(s_u1)
        s_u2[...] = jnp.zeros_like(s_u2)
        s_x[...] = jnp.zeros_like(s_x)
        s_p[...] = jnp.zeros_like(s_p)
        xu_keep[...] = jnp.zeros_like(xu_keep)
        pu_keep[...] = jnp.zeros_like(pu_keep)
        for n in range(3):
            wait_kept(n)
        project(0)
        move(N1, reset_rows, None)
        spread_wait(s_x, 1)
        project(1)
        for n in range(3, 8):
            wait_kept(n)

        def step(i, carry):
            @pl.when(i <= steps)
            def _():
                wait_in(hs.at[0, 0], hs_recv.at[0, lax.rem(i, RING)])

            @pl.when(i < steps)
            def _():
                @pl.when(i > 0)
                def _():
                    spread_wait(s_u1, 0)
                update_part(hs[0, lax.rem(i, RING), :, 0:block], U1, xu_keep, lax.rem(i, 2), s_u1, p_u1, 0, lax.rem(i, RING))

            @pl.when(jnp.logical_and(i >= 1, i <= steps))
            def _():
                h1v = hs[0, lax.rem(i, RING), :, 0:block]

                @pl.when(i > 1)
                def _():
                    spread_wait(s_p, 2)
                s_p[0, :, 0:block] = row_dot(h1v, PR)
                spread(s_p, p_p, 0, 2, lax.rem(i + 3, RING))

            @pl.when(i >= 2)
            def _():
                wait_in(hs.at[1, 0], hs_recv.at[1, lax.rem(i, RING)])

                @pl.when(i > 2)
                def _():
                    spread_wait(s_u2, 3)
                update_part(hs[1, lax.rem(i, RING), :, 0:block], U2, pu_keep, lax.rem(i, 2), s_u2, p_u2, 3, lax.rem(i + 2, RING))

            @pl.when(jnp.logical_and(i >= 1, i <= steps))
            def _():
                s_p[1, :, 0:block] = row_dot(hs[0, lax.rem(i, RING), :, 0:block], PN)
                spread(s_p, p_p, 1, 2, lax.rem(i + 3, RING))

            @pl.when(jnp.logical_and(i >= 1, i <= steps))
            def _():
                pu_keep[lax.rem(i + 1, 2), :, 0:block] = row_dot(hs[0, lax.rem(i, RING), :, 0:block], PU)

            @pl.when(i + 2 < steps)
            def _():
                spread_wait(s_x, 1)
                project(i + 2)

            for n, (u, at) in enumerate(((R2, 0), (N2, 1))):
                @pl.when(i == at)
                def _():
                    move(u, reset_rows, None)
                    wait_in(w_own.at[0, pl.ds(0, nx * rows)], pr_recv.at[n])
                    for tx in range(nx):
                        @pl.when(x != tx)
                        def _():
                            remote(w_own.at[1 + n, pl.ds(tx * rows, rows)], w_own.at[u, partner_rows],
                                   wsend.at[u], wrecv.at[u], tx, 1, y).start()
            return carry

        lax.fori_loop(0, steps + 2, step, 0)
        spread_wait(s_u1, 0)
        spread_wait(s_x, 1)
        spread_wait(s_p, 2)
        spread_wait(s_u2, 3)
        for u in range(4):
            wait_in(w_own.at[0, pl.ds(0, (nx if u in (R1, N1) else 2 * nx - 1) * rows)], wsend.at[u])

        @pl.when(x == y)
        def _():
            wait_in(h0, i_sem.at[0])
        wait_in(out_s, o_sem.at[1])
        wait_in(fin_s, o_sem.at[3])
        seq_out[...] = out_s[...]
        fin_out[...] = fin_s[...]

    @pl.when(core == 1)
    def _():
        fetch_first()
        w_upd[:, :, pl.ds(nx * chunk - LANES, LANES)] = jnp.zeros((2, 2 * rows, LANES), BF16)

        def put(l, row, reset, update):
            w_upd[l, pl.ds(pl.multiple_of(row, 16), 16), 0:block] = update
            w_upd[l, pl.ds(pl.multiple_of(rows + row, 16), 16), 0:block] = reset

        split_gates(put)
        reset_rows = lambda l, j: w_upd.at[l, pl.ds(rows, rows), pl.ds(j * chunk, chunk)]
        pl.semaphore_wait(barrier, 2 * nx * ny - 1)

        @pl.when(x == y)
        def _():
            wait_in(h0s, i_sem.at[1])
            hcat[...] = jnp.zeros_like(hcat)
            hcat[:, :, 0:rows] = h0s[...]
            hcat[:, :, rows:block] = h0[...]
            for d in range(1, nx):
                tx = wrap(x + d, nx)
                remote(hcat.at[:, :, column_slice(tx)], state, i_sem.at[2], i_sem.at[3], tx, 1, y).start()
            state[...] = hcat[:, :, column_slice(x)]
            wait_in(hcat.at[:, :, pl.ds(0, (nx - 1) * chunk)], i_sem.at[2])

        for u in (R1,):
            move(u, reset_rows, wl_sem)
        remote(x_hbm, xb.at[1], x_sem.at[0], x_sem.at[1], x, 0, y).start()
        for src, u in kept:
            if src is None:
                src = w_upd.at[u - U1, pl.ds(0, rows)]
            remote(src, block_weight(u).at[pl.ds(rows, rows)], bs_send.at[u], bs_recv.at[u], x, 0, y).start()
        for n, u in enumerate((R2, N2)):
            for tx in range(nx):
                for src, lanes in pieces(u, tx, reset_rows):
                    remote(src, w_own.at[1 + n, pl.ds(tx * rows, rows), lanes], pr_send.at[n], pr_recv.at[n], x, 0, y).start()

                    @pl.when(x == tx)
                    def _():
                        pltpu.make_async_copy(src, w_own.at[u, my_rows, lanes], wl_sem.at[u]).start()

        for u in range(4):
            w_own[u, pl.ds(nx * block, chunk * nx - block)] = jnp.zeros((chunk * nx - block, chunk), BF16)
        bpad[...] = jnp.zeros_like(bpad)
        bpad[0, 0:3, 0:block] = b1[...]
        bpad[1, 0:3, 0:block] = b2[...]
        bias[...] = bpad[:, :, column_slice(x)]
        valid = jnp.minimum(block - x * chunk, chunk)
        keep = lax.broadcasted_iota(jnp.int32, (batch, chunk), 1) < valid

        @pl.when(x != y)
        def _():
            wait_in(state, i_sem.at[3])

        def to_all(layer, kind):
            for dx, dy in send_order:
                k = offsets.index((dx, dy))
                g = [j for j, (a, b) in enumerate(groups[layer]) if a <= k < b][0]
                remote(ag_buf.at[kind, 0, 0], ag_buf.at[kind, dy, dx], ag_send.at[kind], ag_recv.at[kind, g],
                       wrap(x + dx, nx), 1, wrap(y + dy, ny)).start()

        def to_block(layer, kind, slot):
            dy = wrap(y - x, ny)
            for dx in range(nx):
                remote(ag_buf.at[kind, dy, dx], hs.at[layer, slot, :, column_slice(wrap(x - dx, nx))],
                       hs_send.at[layer], hs_recv.at[layer, slot], x, 0, y).start()

        def chunks(n):
            return w_own.at[0, pl.ds(0, n * batch)]

        def sent(kind):
            wait_in(chunks(peers), ag_send.at[kind])

        def sent_blocks(layer):
            wait_in(chunks(nx), hs_send.at[layer])

        def weight_rows(dx, dy):
            sx, sy = wrap(x - dx, nx), wrap(y - dy, ny)
            return pl.ds(pl.multiple_of(sy * block + sx * chunk, 32), chunk)

        def arrive(layer, kind, g):
            a, b = groups[layer][g]
            wait_in(chunks(b - a), ag_recv.at[kind, g])

        def gathered_dot(layer, kind, u, acc, then=None):
            acc = acc + jnp.dot(ag_buf[kind, 0, 0], w_own[u, weight_rows(0, 0)], preferred_element_type=F32)
            for g, (a, b) in enumerate(groups[layer]):
                arrive(layer, kind, g)
                if g == len(groups[layer]) - 1 and then is not None:
                    then()
                for dx, dy in offsets[a:b]:
                    acc = acc + jnp.dot(ag_buf[kind, dy, dx], w_own[u, weight_rows(dx, dy)], preferred_element_type=F32)
            return acc

        def partial_sum(buf, slot, g):
            total = buf[slot, 0, g]
            for s in range(1, nx):
                total = total + buf[slot, s, g]
            return total

        def wait_weights(u):
            wait_in(w_own.at[u, pl.ds(0, rows)], wl_sem.at[u])
            wait_in(w_own.at[u, pl.ds(0, (2 * nx - 1) * rows)], wrecv.at[u])

        for layer in range(2):
            kind = H1 if layer == 0 else H2
            ag_buf[kind, 0, 0] = jnp.where(keep, state[layer], 0.0).astype(BF16)
            to_all(layer, kind)
        move(N1, reset_rows, wl_sem)

        def copy_row_block(kind):
            blk[:, column_slice(x)] = ag_buf[kind, 0, 0]
            for dx in range(1, nx):
                blk[:, column_slice(wrap(x - dx, nx))] = ag_buf[kind, 0, dx]

        def reset_phase(layer, kind, unit, slot, buf, sem, hslot):
            wait_in(buf.at[0, :, 0], sem.at[0])
            pre = gathered_dot(layer, kind, unit, partial_sum(buf, slot, 0) + bias[layer, 0:1],
                               functools.partial(to_block, layer, kind, hslot))
            if layer == 1:
                copy_row_block(kind)
            gate = jax.nn.sigmoid(pre)
            out = RH1 if layer == 0 else RH2
            ag_buf[out, 0, 0] = jnp.where(keep, gate * state[layer], 0.0).astype(BF16)
            to_all(layer, out)
            sent(kind)

        def candidate_phase(layer, unit, slot, buf, ubuf, usem):
            kind = RH1 if layer == 0 else RH2
            wait_in(buf.at[0, :, 1], in_recv.at[layer, slot, 1])
            pre = gathered_dot(layer, kind, unit, partial_sum(buf, slot, 1) + bias[layer, 2:3])
            cand = jnp.tanh(pre)
            wait_in(ubuf.at[0], usem)
            upd = jax.nn.sigmoid(partial_sum(ubuf, slot, 0) + bias[layer, 1:2])
            new = (1.0 - upd) * cand + upd * state[layer]
            state[layer] = new
            return jnp.where(keep, new, 0.0).astype(BF16)

        part = block // (2 * nx)

        def step(i, carry):
            slot1 = lax.rem(i, RING)
            t2 = i - 2
            slot2 = lax.rem(i + 2, RING)

            @pl.when(i < steps)
            def _():
                @pl.when(i == 0)
                def _():
                    wait_weights(R1)
                reset_phase(0, H1 + lax.rem(i, 2), R1, slot1, p_x, in_recv.at[0, slot1], slot1)

            @pl.when(i == steps)
            def _():
                kind = H1 + lax.rem(i, 2)
                for g in range(len(groups[0])):
                    arrive(0, kind, g)
                to_block(0, kind, slot1)
                sent(kind)

            @pl.when(t2 >= 0)
            def _():
                @pl.when(t2 == 0)
                def _():
                    wait_weights(R2)
                reset_phase(1, H2 + lax.rem(i, 2), R2, slot2, p_p, in_recv.at[1, slot2], slot1)

                @pl.when(t2 >= 1)
                def _():
                    for k in range(nx):
                        @pl.when(x == k)
                        def _():
                            out_s[t2 - 1] = blk[:, 2 * k * part:(2 * k + 1) * part]
                            out_n[t2 - 1] = blk[:, (2 * k + 1) * part:(2 * k + 2) * part]

            @pl.when(i < steps)
            def _():
                @pl.when(i == 0)
                def _():
                    wait_weights(N1)
                new = candidate_phase(0, N1, slot1, p_x, p_u1, rs_recv.at[0, slot1])
                ag_buf[H1 + lax.rem(i + 1, 2), 0, 0] = new
                to_all(0, H1 + lax.rem(i + 1, 2))
                sent(RH1)
                sent_blocks(0)

            @pl.when(t2 >= 0)
            def _():
                @pl.when(t2 == 0)
                def _():
                    wait_weights(N2)
                new = candidate_phase(1, N2, slot2, p_p, p_u2, rs_recv.at[3, slot2])

                @pl.when(t2 < steps - 1)
                def _():
                    ag_buf[H2 + lax.rem(i + 1, 2), 0, 0] = new
                    to_all(1, H2 + lax.rem(i + 1, 2))
                sent(RH2)
                sent_blocks(1)
            return carry

        lax.fori_loop(0, steps + 2, step, 0)
        sent_blocks(0)

        fin_src[...] = state[...]
        for d in range(1, nx):
            tx = wrap(x + d, nx)
            remote(fin_src, fin_buf.at[d], f_sem.at[0], f_sem.at[1], tx, 1, y).start()
        fblk[:, :, column_slice(x)] = state[...]
        wait_in(fin_buf.at[pl.ds(1, nx - 1)], f_sem.at[1])
        for d in range(1, nx):
            fblk[:, :, column_slice(wrap(x - d, nx))] = fin_buf[d]
        for k in range(nx):
            @pl.when(x == k)
            def _():
                s_part = fblk[:, :, 2 * k * part:(2 * k + 1) * part]
                n_part = fblk[:, :, (2 * k + 1) * part:(2 * k + 2) * part]
                fin_s[...] = s_part
                fin_n[...] = n_part
                out_s[steps - 1] = s_part[1].astype(BF16)
                out_n[steps - 1] = n_part[1].astype(BF16)
        remote(fin_s, fin_s, o_sem.at[2], o_sem.at[3], x, 0, y).start()
        remote(out_s, out_s, o_sem.at[0], o_sem.at[1], x, 0, y).start()
        seq_out[...] = out_n[...]
        fin_out[...] = fin_n[...]
        wait_in(fin_s, o_sem.at[2])
        wait_in(out_s, o_sem.at[0])
        wait_in(fin_buf.at[pl.ds(1, nx - 1)], f_sem.at[0])
        wait_in(xb.at[1], x_sem.at[0])
        for u in (R1, N1):
            wait_in(w_own.at[0, pl.ds(0, (nx - 1) * rows)], wsend.at[u])
        for n in range(2):
            wait_in(w_own.at[0, pl.ds(0, nx * rows)], pr_send.at[n])
        for u in range(8):
            wait_in(block_weight(u).at[pl.ds(rows, rows)], bs_send.at[u])


def solution(mesh):
    nx, ny = mesh.shape["row"] // 2, mesh.shape["col"]
    seq_spec = P(None, "data", "row")
    out_spec = P(None, "data", ("col", "row"))
    wide_spec = P("row", None, "col")
    square_spec = P("row", "col")
    bias_spec = P(None, "col")

    def device_body(x_rows, h_rows, wx_l1, whru_l1, whn_l1, bias_l1, wx_l2, whru_l2, whn_l2, bias_l2):
        steps, batch, rows = x_rows.shape
        cols = whn_l1.shape[1]
        chunk = cdiv(cdiv(cols, nx), LANES) * LANES
        wide = nx * chunk
        part = cols // (2 * nx)
        dims = (steps, batch, rows, cols, nx, ny, chunk)

        peers = nx * ny - 1
        total_rows = nx * cols
        hbm = pl.BlockSpec(memory_space=pl.ANY)
        vmem = pl.BlockSpec(memory_space=pltpu.VMEM)
        dma = pltpu.SemaphoreType.DMA
        operands = []
        specs = []
        for lead, wx, wru, wn, b in (((x_rows, h_rows), wx_l1, whru_l1, whn_l1, bias_l1), ((), wx_l2, whru_l2, whn_l2, bias_l2)):
            if lead:
                operands += list(lead)
                specs += [hbm, vmem]
            operands += [jnp.transpose(wx, (1, 0, 2)), wru, wn, b]
            specs += [hbm, hbm, hbm, vmem]
        scratch = [
            pltpu.VMEM((4, total_rows + wide - cols, chunk), BF16),
            pltpu.VMEM((6, 2 * rows, cols), BF16),
            pltpu.VMEM((2, 2 * rows, wide), BF16),
            pltpu.VMEM((2, steps, batch, rows), BF16),
            pltpu.VMEM((2, batch, wide), F32),
            pltpu.VMEM((2, batch, rows), F32),
            pltpu.VMEM((2, batch, chunk), F32),
            pltpu.VMEM((6, ny, nx, batch, chunk), BF16),
            pltpu.VMEM((2, RING, batch, wide), BF16),
            pltpu.VMEM((2, 8, chunk), F32),
            pltpu.VMEM((2, 8, wide), F32),
            pltpu.VMEM((RING, nx, 1, batch, chunk), F32),
            pltpu.VMEM((RING, nx, 2, batch, chunk), F32),
            pltpu.VMEM((RING, nx, 2, batch, chunk), F32),
            pltpu.VMEM((RING, nx, 1, batch, chunk), F32),
            pltpu.VMEM((1, batch, wide), F32),
            pltpu.VMEM((2, batch, wide), F32),
            pltpu.VMEM((2, batch, wide), F32),
            pltpu.VMEM((1, batch, wide), F32),
            pltpu.VMEM((2, batch, wide), F32),
            pltpu.VMEM((2, batch, wide), F32),
            pltpu.VMEM((2, rows // 3, 2, cols), BF16),
            pltpu.VMEM((2, rows // 3, cols), BF16),
            pltpu.VMEM((2, rows, LANES), BF16),
            pltpu.VMEM((batch, wide), BF16),
            pltpu.VMEM((steps, batch, part), BF16),
            pltpu.VMEM((steps, batch, part), BF16),
            pltpu.VMEM((2, batch, chunk), F32),
            pltpu.VMEM((nx, 2, batch, chunk), F32),
            pltpu.VMEM((2, batch, wide), F32),
            pltpu.VMEM((2, batch, part), F32),
            pltpu.VMEM((2, batch, part), F32),
            dma((2, 2)),
            dma((8,)),
            dma((4,)),
            dma((4,)),
            dma((4,)),
            dma((2,)),
            dma((2,)),
            dma((8,)),
            dma((8,)),
            dma((2,)),
            dma((4,)),
            dma((6,)),
            dma((6, 4)),
            dma((2,)),
            dma((2, RING)),
            dma((4,)),
            dma((4, RING)),
            dma((2, RING, 2)),
            dma((2,)),
            dma((4,)),
        ]
        return pl.pallas_call(
            functools.partial(gru_kernel, dims),
            name="gru",
            out_shape=(
                jax.ShapeDtypeStruct((steps, batch, part), BF16),
                jax.ShapeDtypeStruct((2, batch, part), F32),
            ),
            in_specs=specs,
            out_specs=(vmem, vmem),
            scratch_shapes=scratch,
            compiler_params=pltpu.CompilerParams(
                collective_id=0, has_side_effects=True, vmem_limit_bytes=67_000_000
            ),
        )(*operands)

    return jax.shard_map(
        device_body,
        mesh=mesh,
        in_specs=(seq_spec, seq_spec, wide_spec, wide_spec, square_spec, bias_spec, wide_spec, wide_spec, square_spec, bias_spec),
        out_specs=(out_spec, out_spec),
        check_vma=False,
    )
```

```python
import functools

import jax
import jax.numpy as jnp
from jax import lax
from jax.experimental import pallas as pl
from jax.experimental.pallas import tpu as pltpu
from jax.sharding import PartitionSpec as P

MESH = pl.DeviceIdType.MESH
F32 = jnp.float32
BF16 = jnp.bfloat16
LANES = 128

H1, H2, RH1, RH2 = 0, 2, 4, 5
R1, N1, R2, N2 = range(4)
XR, XU, XN, PR, PU, PN, U1, U2 = range(8)
RING = 4


def cdiv(a, b):
    return -(-a // b)


def hop(d, n):
    return min(d, n - d)


def nx_hops(nx, ny):
    return [hop(dx, nx) + hop(dy, ny) for dx in range(nx) for dy in range(ny) if (dx, dy) != (0, 0)]


def gru_kernel(dims, *refs):
    steps, batch, rows, cols, nx, ny, chunk = dims
    (x_hbm, h0, wx1, wru1, wn1, b1, wx2, wru2, wn2, b2,
     seq_out, fin_out,
     w_own, w_blk, w_upd, xb, hcat, h0s, state, ag_buf, hs, bias, bpad,
     p_u1, p_x, p_p, p_u2, s_u1, s_x, s_p, s_u2, xu_keep, pu_keep,
     raw, raw_n, tail, blk, out_n, out_s, fin_src, fin_buf, fblk, fin_n, fin_s,
     raw_sem, ld_sem, wl_sem, wsend, wrecv, pr_send, pr_recv, bs_send, bs_recv, x_sem, i_sem,
     ag_send, ag_recv, hs_send, hs_recv, rs_send, rs_recv, in_recv, f_sem, o_sem) = refs
    block = 2 * rows
    device_row = lax.axis_index("row")
    y = lax.axis_index("col")
    x = device_row // 2
    core = lax.rem(device_row, 2)

    def wrap(v, n):
        return lax.rem(v + n, n)

    def remote(src, dst, ssem, rsem, tx, tc, ty):
        return pltpu.make_async_remote_copy(
            src_ref=src, dst_ref=dst, send_sem=ssem, recv_sem=rsem,
            device_id={"row": tx * 2 + tc, "col": ty}, device_id_type=MESH,
        )

    def wait_in(dst, sem):
        pltpu.make_async_copy(dst, dst, sem).wait()

    offsets = [(dx, dy) for dx in range(nx) for dy in range(ny) if (dx, dy) != (0, 0)]
    offsets.sort(key=lambda o: hop(o[0], nx) + hop(o[1], ny))
    groups = ([(0, 4), (4, 8), (8, 15)], [(0, 5), (5, 15)])
    peers = len(offsets)
    send_order = sorted(
        (o for o in offsets if o[0] and o[1]), key=lambda o: (-hop(o[0], nx) - hop(o[1], ny), -hop(o[1], ny), o[1], o[0]))
    send_order += sorted((o for o in offsets if not o[1]), key=lambda o: (hop(o[0], nx), o[0]))
    send_order += sorted((o for o in offsets if not o[0]), key=lambda o: (-hop(o[1], ny), o[1]))

    barrier = pltpu.get_barrier_semaphore()
    for d in range(1, 2 * nx * ny):
        tr = lax.rem(device_row + d % (2 * nx), 2 * nx)
        ty = lax.rem(y + d // (2 * nx), ny)
        pl.semaphore_signal(barrier, inc=1, device_id={"row": tr, "col": ty}, device_id_type=MESH)

    kept = ((wx1.at[0], XR), (wx1.at[2], XN), (wx1.at[1], XU), (None, U1),
            (wx2.at[0], PR), (wx2.at[2], PN), (wx2.at[1], PU), (None, U2))
    main = (block - (nx - 1) * chunk) // LANES * LANES

    def block_weight(u):
        return w_blk.at[u] if u < U1 else w_upd.at[u - U1]

    my_rows = pl.ds(pl.multiple_of(device_row * rows, 16), rows)

    def column_slice(i):
        return pl.ds(pl.multiple_of(i * chunk, LANES), chunk)

    size = raw.shape[1]
    jobs = [(l, n) for l in range(2) for n in range(rows // size)]

    def fetch(srcs, buf, sem, k):
        l, n = jobs[k]
        return pltpu.make_async_copy(srcs[l].at[pl.ds(n * size, size)], buf.at[k % 2], raw_sem.at[sem, k % 2])

    def fetch_first():
        for k in range(2):
            fetch((wru1, wru2), raw, 0, k).start()
            fetch((wn1, wn2), raw_n, 1, k).start()

    def split_gates(put):
        for k, (l, n) in enumerate(jobs):
            fetch((wru1, wru2), raw, 0, k).wait()

            def some(m, carry):
                both = jnp.transpose(raw[k % 2, pl.ds(pl.multiple_of(m * 16, 16), 16)], (1, 0, 2))
                put(l, n * size + m * 16, both[0], both[1])
                return carry
            lax.fori_loop(0, size // 16, some, 0)
            if k + 2 < len(jobs):
                fetch((wru1, wru2), raw, 0, k + 2).start()
            fetch((wn1, wn2), raw_n, 1, k).wait()
            rest = raw_n[k % 2, :, (nx - 1) * chunk + main:]
            tail[l, pl.ds(n * size, size)] = jnp.concatenate([rest, jnp.zeros((size, LANES - rest.shape[1]), BF16)], axis=1)
            if k + 2 < len(jobs):
                fetch((wn1, wn2), raw_n, 1, k + 2).start()

    def pieces(u, j, reset_source):
        l = 0 if u in (R1, N1) else 1
        if u in (R1, R2):
            return [(reset_source(l, j), pl.ds(0, chunk))]
        src = (wn1, wn2)[l]
        if j < nx - 1:
            return [(src.at[:, pl.ds(j * chunk, chunk)], pl.ds(0, chunk))]
        return [(src.at[:, pl.ds(j * chunk, main)], pl.ds(0, main)), (tail.at[l], pl.ds(main, LANES))]

    def move(u, reset_source, to_self):
        for tx in range(nx):
            for src, lanes in pieces(u, tx, reset_source):
                dst = w_own.at[u, my_rows, lanes]
                if to_self is None:
                    remote(src, dst, wsend.at[u], wrecv.at[u], tx, 1, y).start()
                else:
                    @pl.when(x != tx)
                    def _():
                        remote(src, dst, wsend.at[u], wrecv.at[u], tx, 1, y).start()

                    @pl.when(x == tx)
                    def _():
                        pltpu.make_async_copy(src, dst, to_self.at[u]).start()

    @pl.when(core == 0)
    def _():
        partner_rows = pl.ds(pl.multiple_of((device_row + 1) * rows, 16), rows)
        fetch_first()
        spare = lambda l, j: (nx * l + j) * rows
        w_upd[:, pl.ds(0, rows), pl.ds(nx * chunk - LANES, LANES)] = jnp.zeros((2, rows, LANES), BF16)
        for l in range(2):
            w_own[0, pl.ds(spare(l, nx - 1), rows), pl.ds(chunk - LANES, LANES)] = jnp.zeros((rows, LANES), BF16)

        def put(l, row, reset, update):
            w_upd[l, pl.ds(pl.multiple_of(row, 16), 16), 0:block] = update
            for j in range(nx):
                width = min(chunk, block - j * chunk)
                w_own[0, pl.ds(pl.multiple_of(spare(l, j) + row, 16), 16), 0:width] = reset[:, j * chunk:j * chunk + width]

        split_gates(put)
        reset_rows = lambda l, j: w_own.at[0, pl.ds(spare(l, j), rows)]
        xload = pltpu.make_async_copy(x_hbm, xb.at[0], x_sem.at[0])
        xload.start()
        for src, u in kept:
            if src is not None:
                pltpu.make_async_copy(src, block_weight(u).at[pl.ds(0, rows)], ld_sem.at[u]).start()
        pl.semaphore_wait(barrier, 2 * nx * ny - 1)

        @pl.when(x == y)
        def _():
            remote(h0, h0s, i_sem.at[0], i_sem.at[1], x, 1, y).start()

        move(R1, reset_rows, None)

        xload.wait()
        wait_in(xb.at[1], x_sem.at[1])

        def wait_kept(n):
            u = kept[n][1]
            if u < U1:
                wait_in(block_weight(u).at[pl.ds(0, rows)], ld_sem.at[u])
            wait_in(block_weight(u).at[pl.ds(rows, rows)], bs_recv.at[u])

        def row_dot(vec, u):
            return jnp.dot(vec, block_weight(u)[:, 0:block], preferred_element_type=F32)

        near_last = sorted(range(nx), key=lambda d: (-hop(d, nx), -d))

        def spread(src, dst, g, kind, slot):
            for d in near_last:
                tx = wrap(x + d, nx)
                remote(src.at[g, :, column_slice(tx)], dst.at[slot, x, g], rs_send.at[kind], in_recv.at[kind - 1, slot, g], tx, 1, y).start()

        def update_part(vec, u, kept_sum, kept_slot, src, dst, kind, slot):
            for d in near_last:
                tx = wrap(x + d, nx)
                src[0, :, column_slice(tx)] = (
                    jnp.dot(vec, block_weight(u)[:, column_slice(tx)], preferred_element_type=F32)
                    + kept_sum[kept_slot, :, column_slice(tx)])
                remote(src.at[:, :, column_slice(tx)], dst.at[slot, x], rs_send.at[kind], rs_recv.at[kind, slot], tx, 1, y).start()

        def spread_wait(src, kind):
            wait_in(src, rs_send.at[kind])

        def project(t):
            def half(g):
                return (jnp.dot(xb[0, t], w_blk[g, 0:rows], preferred_element_type=F32)
                        + jnp.dot(xb[1, t], w_blk[g, rows:block], preferred_element_type=F32))
            for g, u in enumerate((XR, XN)):
                s_x[g, :, 0:block] = half(u)
                spread(s_x, p_x, g, 1, lax.rem(t, RING))
            xu_keep[lax.rem(t, 2), :, 0:block] = half(XU)

        s_u1[...] = jnp.zeros_like(s_u1)
        s_u2[...] = jnp.zeros_like(s_u2)
        s_x[...] = jnp.zeros_like(s_x)
        s_p[...] = jnp.zeros_like(s_p)
        xu_keep[...] = jnp.zeros_like(xu_keep)
        pu_keep[...] = jnp.zeros_like(pu_keep)
        for n in range(3):
            wait_kept(n)
        project(0)
        move(N1, reset_rows, None)
        spread_wait(s_x, 1)
        project(1)
        for n in range(3, 8):
            wait_kept(n)

        def step(i, carry):
            @pl.when(i <= steps)
            def _():
                wait_in(hs.at[0, 0], hs_recv.at[0, lax.rem(i, RING)])

            @pl.when(i < steps)
            def _():
                @pl.when(i > 0)
                def _():
                    spread_wait(s_u1, 0)
                update_part(hs[0, lax.rem(i, RING), :, 0:block], U1, xu_keep, lax.rem(i, 2), s_u1, p_u1, 0, lax.rem(i, RING))

            @pl.when(jnp.logical_and(i >= 1, i <= steps))
            def _():
                h1v = hs[0, lax.rem(i, RING), :, 0:block]

                @pl.when(i > 1)
                def _():
                    spread_wait(s_p, 2)
                s_p[0, :, 0:block] = row_dot(h1v, PR)
                spread(s_p, p_p, 0, 2, lax.rem(i + 3, RING))

            @pl.when(i >= 2)
            def _():
                wait_in(hs.at[1, 0], hs_recv.at[1, lax.rem(i, RING)])

                @pl.when(i > 2)
                def _():
                    spread_wait(s_u2, 3)
                update_part(hs[1, lax.rem(i, RING), :, 0:block], U2, pu_keep, lax.rem(i, 2), s_u2, p_u2, 3, lax.rem(i + 2, RING))

            @pl.when(jnp.logical_and(i >= 1, i <= steps))
            def _():
                s_p[1, :, 0:block] = row_dot(hs[0, lax.rem(i, RING), :, 0:block], PN)
                spread(s_p, p_p, 1, 2, lax.rem(i + 3, RING))

            @pl.when(jnp.logical_and(i >= 1, i <= steps))
            def _():
                pu_keep[lax.rem(i + 1, 2), :, 0:block] = row_dot(hs[0, lax.rem(i, RING), :, 0:block], PU)

            @pl.when(i + 2 < steps)
            def _():
                spread_wait(s_x, 1)
                project(i + 2)

            for n, (u, at) in enumerate(((R2, 0), (N2, 1))):
                @pl.when(i == at)
                def _():
                    move(u, reset_rows, None)
                    wait_in(w_own.at[0, pl.ds(0, nx * rows)], pr_recv.at[n])
                    for tx in range(nx):
                        @pl.when(x != tx)
                        def _():
                            remote(w_own.at[1 + n, pl.ds(tx * rows, rows)], w_own.at[u, partner_rows],
                                   wsend.at[u], wrecv.at[u], tx, 1, y).start()
            return carry

        lax.fori_loop(0, steps + 2, step, 0)
        spread_wait(s_u1, 0)
        spread_wait(s_x, 1)
        spread_wait(s_p, 2)
        spread_wait(s_u2, 3)
        for u in range(4):
            wait_in(w_own.at[0, pl.ds(0, (nx if u in (R1, N1) else 2 * nx - 1) * rows)], wsend.at[u])

        @pl.when(x == y)
        def _():
            wait_in(h0, i_sem.at[0])
        wait_in(out_s, o_sem.at[1])
        wait_in(fin_s, o_sem.at[3])
        seq_out[...] = out_s[...]
        fin_out[...] = fin_s[...]

    @pl.when(core == 1)
    def _():
        fetch_first()
        w_upd[:, :, pl.ds(nx * chunk - LANES, LANES)] = jnp.zeros((2, 2 * rows, LANES), BF16)

        def put(l, row, reset, update):
            w_upd[l, pl.ds(pl.multiple_of(row, 16), 16), 0:block] = update
            w_upd[l, pl.ds(pl.multiple_of(rows + row, 16), 16), 0:block] = reset

        split_gates(put)
        reset_rows = lambda l, j: w_upd.at[l, pl.ds(rows, rows), pl.ds(j * chunk, chunk)]
        pl.semaphore_wait(barrier, 2 * nx * ny - 1)

        @pl.when(x == y)
        def _():
            wait_in(h0s, i_sem.at[1])
            hcat[...] = jnp.zeros_like(hcat)
            hcat[:, :, 0:rows] = h0s[...]
            hcat[:, :, rows:block] = h0[...]
            for d in range(1, nx):
                tx = wrap(x + d, nx)
                remote(hcat.at[:, :, column_slice(tx)], state, i_sem.at[2], i_sem.at[3], tx, 1, y).start()
            state[...] = hcat[:, :, column_slice(x)]
            wait_in(hcat.at[:, :, pl.ds(0, (nx - 1) * chunk)], i_sem.at[2])

        for u in (R1,):
            move(u, reset_rows, wl_sem)
        remote(x_hbm, xb.at[1], x_sem.at[0], x_sem.at[1], x, 0, y).start()
        for src, u in kept:
            if src is None:
                src = w_upd.at[u - U1, pl.ds(0, rows)]
            remote(src, block_weight(u).at[pl.ds(rows, rows)], bs_send.at[u], bs_recv.at[u], x, 0, y).start()
        for n, u in enumerate((R2, N2)):
            for tx in range(nx):
                for src, lanes in pieces(u, tx, reset_rows):
                    remote(src, w_own.at[1 + n, pl.ds(tx * rows, rows), lanes], pr_send.at[n], pr_recv.at[n], x, 0, y).start()

                    @pl.when(x == tx)
                    def _():
                        pltpu.make_async_copy(src, w_own.at[u, my_rows, lanes], wl_sem.at[u]).start()

        for u in range(4):
            w_own[u, pl.ds(nx * block, chunk * nx - block)] = jnp.zeros((chunk * nx - block, chunk), BF16)
        bpad[...] = jnp.zeros_like(bpad)
        bpad[0, 0:3, 0:block] = b1[...]
        bpad[1, 0:3, 0:block] = b2[...]
        bias[...] = bpad[:, :, column_slice(x)]
        valid = jnp.minimum(block - x * chunk, chunk)
        keep = lax.broadcasted_iota(jnp.int32, (batch, chunk), 1) < valid

        @pl.when(x != y)
        def _():
            wait_in(state, i_sem.at[3])

        def to_all(layer, kind):
            for dx, dy in send_order:
                k = offsets.index((dx, dy))
                g = [j for j, (a, b) in enumerate(groups[layer]) if a <= k < b][0]
                remote(ag_buf.at[kind, 0, 0], ag_buf.at[kind, dy, dx], ag_send.at[kind], ag_recv.at[kind, g],
                       wrap(x + dx, nx), 1, wrap(y + dy, ny)).start()

        def to_block(layer, kind, slot):
            dy = wrap(y - x, ny)
            for dx in range(nx):
                remote(ag_buf.at[kind, dy, dx], hs.at[layer, slot, :, column_slice(wrap(x - dx, nx))],
                       hs_send.at[layer], hs_recv.at[layer, slot], x, 0, y).start()

        def chunks(n):
            return w_own.at[0, pl.ds(0, n * batch)]

        def sent(kind):
            wait_in(chunks(peers), ag_send.at[kind])

        def sent_blocks(layer):
            wait_in(chunks(nx), hs_send.at[layer])

        def weight_rows(dx, dy):
            sx, sy = wrap(x - dx, nx), wrap(y - dy, ny)
            return pl.ds(pl.multiple_of(sy * block + sx * chunk, 32), chunk)

        def arrive(layer, kind, g):
            a, b = groups[layer][g]
            wait_in(chunks(b - a), ag_recv.at[kind, g])

        def gathered_dot(layer, kind, u, acc, then=None):
            acc = acc + jnp.dot(ag_buf[kind, 0, 0], w_own[u, weight_rows(0, 0)], preferred_element_type=F32)
            for g, (a, b) in enumerate(groups[layer]):
                arrive(layer, kind, g)
                if g == len(groups[layer]) - 1 and then is not None:
                    then()
                for dx, dy in offsets[a:b]:
                    acc = acc + jnp.dot(ag_buf[kind, dy, dx], w_own[u, weight_rows(dx, dy)], preferred_element_type=F32)
            return acc

        def partial_sum(buf, slot, g):
            total = buf[slot, 0, g]
            for s in range(1, nx):
                total = total + buf[slot, s, g]
            return total

        def wait_weights(u):
            wait_in(w_own.at[u, pl.ds(0, rows)], wl_sem.at[u])
            wait_in(w_own.at[u, pl.ds(0, (2 * nx - 1) * rows)], wrecv.at[u])

        for layer in range(2):
            kind = H1 if layer == 0 else H2
            ag_buf[kind, 0, 0] = jnp.where(keep, state[layer], 0.0).astype(BF16)
            to_all(layer, kind)
        move(N1, reset_rows, wl_sem)

        def copy_row_block(kind):
            blk[:, column_slice(x)] = ag_buf[kind, 0, 0]
            for dx in range(1, nx):
                blk[:, column_slice(wrap(x - dx, nx))] = ag_buf[kind, 0, dx]

        def reset_phase(layer, kind, unit, slot, buf, sem, hslot):
            wait_in(buf.at[0, :, 0], sem.at[0])
            pre = gathered_dot(layer, kind, unit, partial_sum(buf, slot, 0) + bias[layer, 0:1],
                               functools.partial(to_block, layer, kind, hslot))
            if layer == 1:
                copy_row_block(kind)
            gate = jax.nn.sigmoid(pre)
            out = RH1 if layer == 0 else RH2
            ag_buf[out, 0, 0] = jnp.where(keep, gate * state[layer], 0.0).astype(BF16)
            to_all(layer, out)
            sent(kind)

        def candidate_phase(layer, unit, slot, buf, ubuf, usem):
            kind = RH1 if layer == 0 else RH2
            wait_in(buf.at[0, :, 1], in_recv.at[layer, slot, 1])
            pre = gathered_dot(layer, kind, unit, partial_sum(buf, slot, 1) + bias[layer, 2:3])
            cand = jnp.tanh(pre)
            wait_in(ubuf.at[0], usem)
            upd = jax.nn.sigmoid(partial_sum(ubuf, slot, 0) + bias[layer, 1:2])
            new = (1.0 - upd) * cand + upd * state[layer]
            state[layer] = new
            return jnp.where(keep, new, 0.0).astype(BF16)

        part = block // (2 * nx)

        def step(i, carry):
            slot1 = lax.rem(i, RING)
            t2 = i - 2
            slot2 = lax.rem(i + 2, RING)

            @pl.when(i < steps)
            def _():
                @pl.when(i == 0)
                def _():
                    wait_weights(R1)
                reset_phase(0, H1 + lax.rem(i, 2), R1, slot1, p_x, in_recv.at[0, slot1], slot1)

            @pl.when(i == steps)
            def _():
                kind = H1 + lax.rem(i, 2)
                for g in range(len(groups[0])):
                    arrive(0, kind, g)
                to_block(0, kind, slot1)
                sent(kind)

            @pl.when(t2 >= 0)
            def _():
                @pl.when(t2 == 0)
                def _():
                    wait_weights(R2)
                reset_phase(1, H2 + lax.rem(i, 2), R2, slot2, p_p, in_recv.at[1, slot2], slot1)

                @pl.when(t2 >= 1)
                def _():
                    for k in range(nx):
                        @pl.when(x == k)
                        def _():
                            out_s[t2 - 1] = blk[:, 2 * k * part:(2 * k + 1) * part]
                            out_n[t2 - 1] = blk[:, (2 * k + 1) * part:(2 * k + 2) * part]

            @pl.when(i < steps)
            def _():
                @pl.when(i == 0)
                def _():
                    wait_weights(N1)
                new = candidate_phase(0, N1, slot1, p_x, p_u1, rs_recv.at[0, slot1])
                ag_buf[H1 + lax.rem(i + 1, 2), 0, 0] = new
                to_all(0, H1 + lax.rem(i + 1, 2))
                sent(RH1)
                sent_blocks(0)

            @pl.when(t2 >= 0)
            def _():
                @pl.when(t2 == 0)
                def _():
                    wait_weights(N2)
                new = candidate_phase(1, N2, slot2, p_p, p_u2, rs_recv.at[3, slot2])

                @pl.when(t2 < steps - 1)
                def _():
                    ag_buf[H2 + lax.rem(i + 1, 2), 0, 0] = new
                    to_all(1, H2 + lax.rem(i + 1, 2))
                sent(RH2)
                sent_blocks(1)
            return carry

        lax.fori_loop(0, steps + 2, step, 0)
        sent_blocks(0)

        fin_src[...] = state[...]
        for d in range(1, nx):
            tx = wrap(x + d, nx)
            remote(fin_src, fin_buf.at[d], f_sem.at[0], f_sem.at[1], tx, 1, y).start()
        fblk[:, :, column_slice(x)] = state[...]
        wait_in(fin_buf.at[pl.ds(1, nx - 1)], f_sem.at[1])
        for d in range(1, nx):
            fblk[:, :, column_slice(wrap(x - d, nx))] = fin_buf[d]
        for k in range(nx):
            @pl.when(x == k)
            def _():
                s_part = fblk[:, :, 2 * k * part:(2 * k + 1) * part]
                n_part = fblk[:, :, (2 * k + 1) * part:(2 * k + 2) * part]
                fin_s[...] = s_part
                fin_n[...] = n_part
                out_s[steps - 1] = s_part[1].astype(BF16)
                out_n[steps - 1] = n_part[1].astype(BF16)
        remote(fin_s, fin_s, o_sem.at[2], o_sem.at[3], x, 0, y).start()
        remote(out_s, out_s, o_sem.at[0], o_sem.at[1], x, 0, y).start()
        seq_out[...] = out_n[...]
        fin_out[...] = fin_n[...]
        wait_in(fin_s, o_sem.at[2])
        wait_in(out_s, o_sem.at[0])
        wait_in(fin_buf.at[pl.ds(1, nx - 1)], f_sem.at[0])
        wait_in(xb.at[1], x_sem.at[0])
        for u in (R1, N1):
            wait_in(w_own.at[0, pl.ds(0, (nx - 1) * rows)], wsend.at[u])
        for n in range(2):
            wait_in(w_own.at[0, pl.ds(0, nx * rows)], pr_send.at[n])
        for u in range(8):
            wait_in(block_weight(u).at[pl.ds(rows, rows)], bs_send.at[u])


def solution(mesh):
    nx, ny = mesh.shape["row"] // 2, mesh.shape["col"]
    seq_spec = P(None, "data", "row")
    out_spec = P(None, "data", ("col", "row"))
    wide_spec = P("row", None, "col")
    square_spec = P("row", "col")
    bias_spec = P(None, "col")

    def device_body(x_rows, h_rows, wx_l1, whru_l1, whn_l1, bias_l1, wx_l2, whru_l2, whn_l2, bias_l2):
        steps, batch, rows = x_rows.shape
        cols = whn_l1.shape[1]
        chunk = cdiv(cdiv(cols, nx), LANES) * LANES
        wide = nx * chunk
        part = cols // (2 * nx)
        dims = (steps, batch, rows, cols, nx, ny, chunk)

        peers = nx * ny - 1
        total_rows = nx * cols
        hbm = pl.BlockSpec(memory_space=pl.ANY)
        vmem = pl.BlockSpec(memory_space=pltpu.VMEM)
        dma = pltpu.SemaphoreType.DMA
        operands = []
        specs = []
        for lead, wx, wru, wn, b in (((x_rows, h_rows), wx_l1, whru_l1, whn_l1, bias_l1), ((), wx_l2, whru_l2, whn_l2, bias_l2)):
            if lead:
                operands += list(lead)
                specs += [hbm, vmem]
            operands += [jnp.transpose(wx, (1, 0, 2)), wru, wn, b]
            specs += [hbm, hbm, hbm, vmem]
        scratch = [
            pltpu.VMEM((4, total_rows + wide - cols, chunk), BF16),
            pltpu.VMEM((6, 2 * rows, cols), BF16),
            pltpu.VMEM((2, 2 * rows, wide), BF16),
            pltpu.VMEM((2, steps, batch, rows), BF16),
            pltpu.VMEM((2, batch, wide), F32),
            pltpu.VMEM((2, batch, rows), F32),
            pltpu.VMEM((2, batch, chunk), F32),
            pltpu.VMEM((6, ny, nx, batch, chunk), BF16),
            pltpu.VMEM((2, RING, batch, wide), BF16),
            pltpu.VMEM((2, 8, chunk), F32),
            pltpu.VMEM((2, 8, wide), F32),
            pltpu.VMEM((RING, nx, 1, batch, chunk), F32),
            pltpu.VMEM((RING, nx, 2, batch, chunk), F32),
            pltpu.VMEM((RING, nx, 2, batch, chunk), F32),
            pltpu.VMEM((RING, nx, 1, batch, chunk), F32),
            pltpu.VMEM((1, batch, wide), F32),
            pltpu.VMEM((2, batch, wide), F32),
            pltpu.VMEM((2, batch, wide), F32),
            pltpu.VMEM((1, batch, wide), F32),
            pltpu.VMEM((2, batch, wide), F32),
            pltpu.VMEM((2, batch, wide), F32),
            pltpu.VMEM((2, rows // 3, 2, cols), BF16),
            pltpu.VMEM((2, rows // 3, cols), BF16),
            pltpu.VMEM((2, rows, LANES), BF16),
            pltpu.VMEM((batch, wide), BF16),
            pltpu.VMEM((steps, batch, part), BF16),
            pltpu.VMEM((steps, batch, part), BF16),
            pltpu.VMEM((2, batch, chunk), F32),
            pltpu.VMEM((nx, 2, batch, chunk), F32),
            pltpu.VMEM((2, batch, wide), F32),
            pltpu.VMEM((2, batch, part), F32),
            pltpu.VMEM((2, batch, part), F32),
            dma((2, 2)),
            dma((8,)),
            dma((4,)),
            dma((4,)),
            dma((4,)),
            dma((2,)),
            dma((2,)),
            dma((8,)),
            dma((8,)),
            dma((2,)),
            dma((4,)),
            dma((6,)),
            dma((6, 4)),
            dma((2,)),
            dma((2, RING)),
            dma((4,)),
            dma((4, RING)),
            dma((2, RING, 2)),
            dma((2,)),
            dma((4,)),
        ]
        return pl.pallas_call(
            functools.partial(gru_kernel, dims),
            name="gru",
            out_shape=(
                jax.ShapeDtypeStruct((steps, batch, part), BF16),
                jax.ShapeDtypeStruct((2, batch, part), F32),
            ),
            in_specs=specs,
            out_specs=(vmem, vmem),
            scratch_shapes=scratch,
            compiler_params=pltpu.CompilerParams(
                collective_id=0, has_side_effects=True, vmem_limit_bytes=67_000_000
            ),
        )(*operands)

    return jax.shard_map(
        device_body,
        mesh=mesh,
        in_specs=(seq_spec, seq_spec, wide_spec, wide_spec, square_spec, bias_spec, wide_spec, wide_spec, square_spec, bias_spec),
        out_specs=(out_spec, out_spec),
        check_vma=False,
    )
```
